128 devices in a mesh: day: 16 (over x, y), pair: 8 (over z, core).
Axes of the slice: x: 4, y: 4, z: 4, core: 2. Of those that a mesh axis runs over, the one named last changes fastest.
Arguments:
- correlations: bfloat16 [64, 4096, 2001], P('day', 'pair'), may hold values from -8 to 8
- mask: int32 [64, 4096], P('day', 'pair'), may hold values from 0 to 1, as said below
- counts: int32 [4096], P(('pair', 'day')), may hold values from 1 to 64, as said below
Outputs:
- phase_weighted: float32 [4096, 2001], P(('pair', 'day'))
- linear: float32 [4096, 2001], P(('pair', 'day'))
The draws below stay inside these ranges and needn't reach their ends.
Inputs may be any that keep to these rules, and one draw needn't show every extreme that they name: `mask`: every pair has a usable correlation on at least one day. counts[p] equals the number of days d with mask[d, p] = 1.
All inputs are finite; a program needn't handle non-finite values.
Results may differ from the reference program's by a relative error of at most 0.00044.
Values may be sent and summed in bfloat16 or wider, within the bound.
No kernel may reach another device: no remote copies, remote signals or barrier semaphores. Data moves between devices by JAX's collectives and lax.ppermute only.
A program may use at most 128 MiB of HBM per device.

```python
import jax
import jax.numpy as jnp
from jax import lax

LAGS = 2001
DAYS = 64
PAIRS = 4096


def mask_pair(key):
    base = jax.random.fold_in(key, 7)
    keys = jax.random.split(base, 5)
    day_rate = jax.random.randint(keys[0], (DAYS,), 30, 101)
    pair_rate = jax.random.randint(keys[1], (PAIRS,), 40, 101)
    draws = jax.random.randint(keys[2], (DAYS, PAIRS), 0, 10000)
    usable = (draws < day_rate[:, None] * pair_rate[None, :]).astype(jnp.int32)
    forced = jax.random.randint(keys[3], (PAIRS,), 0, DAYS)
    chosen = (jnp.arange(DAYS)[:, None] == forced[None, :]).astype(jnp.int32)
    usable = jnp.maximum(usable, chosen)
    full_pair = jax.random.randint(keys[4], (), 0, PAIRS)
    always = (jnp.arange(PAIRS) == full_pair).astype(jnp.int32)
    usable = jnp.maximum(usable, always[None, :])
    return (usable, jnp.sum(usable, axis=0).astype(jnp.int32))


def draw_mask(key, part):
    return mask_pair(key)[0]


def draw_counts(key, part):
    return mask_pair(key)[1]


def draw_correlations(key, part):
    keys = jax.random.split(jax.random.fold_in(key, 3), 5)
    block_index = jnp.arange(PAIRS) // 64
    block_total = (PAIRS + 63) // 64
    pair_scale = jnp.exp(jax.random.uniform(keys[0], (PAIRS,), jnp.float32, -0.8, 0.8))
    block_scale = jnp.exp(jax.random.uniform(keys[1], (block_total,), jnp.float32, -0.8, 0.8))[block_index]
    day_scale = jnp.exp(jax.random.uniform(keys[2], (DAYS,), jnp.float32, -0.7, 0.7))
    signal = 0.7 * jax.random.normal(keys[3], (PAIRS, LAGS), jnp.float32)
    noise = jax.random.normal(keys[4], (DAYS, PAIRS, LAGS), jnp.float32)
    values = day_scale[:, None, None] * (pair_scale * block_scale)[None, :, None] * (signal[None] + noise)
    return jnp.clip(values, -8.0, 8.0).astype(jnp.bfloat16)


def setup_inputs(seed: int = 0) -> dict:
    seeds = jax.random.split(jax.random.key(seed), 4)
    correlations = draw_correlations(jax.random.fold_in(seeds[3], 71), 0)
    mask = draw_mask(jax.random.fold_in(seeds[3], 71), 0)
    counts = draw_counts(jax.random.fold_in(seeds[3], 71), 0)
    return dict(correlations=correlations, mask=mask, counts=counts)


def hilbert_kernel():
    offset = jnp.arange(LAGS, dtype=jnp.int32)
    offset = jnp.where(offset > LAGS // 2, offset - LAGS, offset)
    phase_angle = jnp.pi * offset.astype(jnp.float32) / LAGS
    parity = 1.0 - 2.0 * (offset % 2).astype(jnp.float32)
    sine_safe = jnp.where(offset == 0, 1.0, jnp.sin(phase_angle))
    kernel = jnp.where(offset == 0, 0.0, (jnp.cos(phase_angle) - parity) / (LAGS * sine_safe))
    rounded = lax.optimization_barrier(kernel.astype(jnp.bfloat16))
    return rounded.astype(jnp.float32)

def hilbert_part(day_rows, kernel_spectrum):
    spectrum = jnp.fft.fft(day_rows, axis=-1)
    return jnp.real(jnp.fft.ifft(spectrum * kernel_spectrum, axis=-1))

def reference(correlations, mask, counts):
    masked = correlations * mask[:, :, None].astype(jnp.bfloat16)
    energy = lax.map(lambda day_rows: jnp.sum(jnp.square(day_rows.astype(jnp.float32))), masked)
    used_pairs = lax.optimization_barrier(jnp.sum(mask, axis=1)).astype(jnp.float32)
    weight = 1.0 / jnp.sqrt(energy / (LAGS * jnp.maximum(used_pairs, 1.0)) + 0.1)
    kernel_spectrum = jnp.fft.fft(hilbert_kernel())

    def add_day(totals, inputs):
        day_rows, day_weight = inputs
        values = day_rows.astype(jnp.float32)
        real_part = day_weight * values
        imag_part = day_weight * hilbert_part(values, kernel_spectrum)
        amplitude = jnp.sqrt(real_part * real_part + imag_part * imag_part + 0.25)
        return ((totals[0] + real_part, totals[1] + real_part / amplitude, totals[2] + imag_part / amplitude), None)
    zeros = jnp.zeros((PAIRS, LAGS), jnp.float32)
    totals, unused = lax.scan(add_day, (zeros, zeros, zeros), (masked, weight))
    divisor = jnp.maximum(counts.astype(jnp.float32), 1.0)[:, None]
    linear = totals[0] / divisor
    coherence = (totals[1] * totals[1] + totals[2] * totals[2]) / (divisor * divisor)
    return (linear * coherence, linear)
```

```python
import functools

import jax
import jax.numpy as jnp
from jax import lax
from jax.experimental import pallas as pl
from jax.experimental.pallas import tpu as pltpu
from jax.sharding import PartitionSpec as P


LAGS = 2001
WIDTH = 2048
WORDS = WIDTH // 2
OWNED = 32
DAYS = 4
SIDE = 4
QUANTITIES = 3
TOP = 32766.0
KERNEL_SUM = 6.0
MB = 1 << 20

params = functools.partial(pltpu.CompilerParams, vmem_limit_bytes=40 * MB)


def encode(value, scale):
    root = value * lax.rsqrt(jnp.abs(value) + 1e-36)
    return (root * scale + 32768.5).astype(jnp.int32)


def pack(low, high):
    return low | (high << 16)


def unpack(word):
    low = (word & 0xFFFF).astype(jnp.float32) - 32768.0
    high = (lax.shift_right_logical(word, 16)).astype(jnp.float32) - 32768.0
    return low * jnp.abs(low), high * jnp.abs(high)


def unit(exponent):
    return jnp.exp2(exponent.astype(jnp.float32)) * (1.0 / (TOP * TOP))


def table_kernel(ext_ref, out_ref, rolled_ref):
    for q in range(16):
        first = pltpu.roll(ext_ref[...], 16 * q, 1)
        second = pltpu.roll(ext_ref[...], 16 * q + 8, 1)
        rolled_ref[16 * q : 16 * q + 16, :] = jnp.concatenate([first, second], 0).astype(jnp.bfloat16)
    for q in range(8):
        for n in range(8):
            for h in range(2):
                start = 128 * (n + 8 * h) - 256 * q + WIDTH
                out_ref[256 * q : 256 * q + 256, 256 * n + 128 * h : 256 * n + 128 * h + 128] = rolled_ref[
                    :, start : start + 128
                ]


def kernel_table():
    row = lax.broadcasted_iota(jnp.int32, (8, 2 * WIDTH), 0)
    col = lax.broadcasted_iota(jnp.int32, (8, 2 * WIDTH), 1)
    offset = (col - row - WIDTH + 2 * LAGS) % LAGS
    offset = jnp.where(offset > LAGS // 2, offset - LAGS, offset)
    angle = jnp.pi * offset.astype(jnp.float32) / LAGS
    parity = 1.0 - 2.0 * (offset % 2).astype(jnp.float32)
    sine = jnp.where(offset == 0, 1.0, jnp.sin(angle))
    ext = jnp.where(offset == 0, 0.0, (jnp.cos(angle) - parity) / (LAGS * sine))
    ext = ext.astype(jnp.bfloat16).astype(jnp.float32)
    return pl.pallas_call(
        table_kernel,
        out_shape=jax.ShapeDtypeStruct((WIDTH, WIDTH), jnp.bfloat16),
        scratch_shapes=[pltpu.VMEM((256, 2 * WIDTH), jnp.bfloat16)],
        compiler_params=params(),
        name="table",
    )(ext)


def terms_kernel(order_ref, weight_ref, scale_ref, exp_ref, *refs):
    x_refs, (table_ref, out_ref, rows_ref) = refs[:SIDE], refs[SIDE:]
    n = pl.program_id(0)

    @pl.when(n == 0)
    def _():
        lane = lax.broadcasted_iota(jnp.int32, (OWNED, 128), 1)
        for l in range(SIDE):
            for d in range(DAYS):
                at = (l * DAYS + d) * OWNED
                rows_ref[at : at + OWNED, : WIDTH - 128] = x_refs[l][d, :, : WIDTH - 128]
                tail = x_refs[l][d, :, WIDTH - 128 :]
                keep = lane < LAGS - (WIDTH - 128)
                rows_ref[at : at + OWNED, WIDTH - 128 :] = jnp.where(
                    keep, tail.astype(jnp.float32), 0.0
                ).astype(jnp.bfloat16)

    hilbert = jnp.dot(rows_ref[...], table_ref[...], preferred_element_type=jnp.float32)
    for l in range(SIDE):
        codes = []
        for h in range(2):
            lanes = pl.ds(pl.multiple_of(n * 128 + h * WORDS, 128), 128)
            linear = real = imag = None
            for d in range(DAYS):
                at = (l * DAYS + d) * OWNED
                w = weight_ref[d]
                real_part = rows_ref[at : at + OWNED, lanes].astype(jnp.float32) * w
                imag_part = hilbert[at : at + OWNED, 128 * h : 128 * h + 128] * w
                inverse = lax.rsqrt(real_part * real_part + imag_part * imag_part + 0.25)
                a, b = real_part * inverse, imag_part * inverse
                linear = real_part if d == 0 else linear + real_part
                real = a if d == 0 else real + a
                imag = b if d == 0 else imag + b
            codes.append([encode(v, scale_ref[q]) for q, v in enumerate((linear, real, imag))])
        for q in range(QUANTITIES):
            at = (l * QUANTITIES + q) * OWNED
            out_ref[at : at + OWNED, :] = pack(codes[0][q], codes[1][q])
    row = lax.broadcasted_iota(jnp.int32, (8, 128), 0)
    out_ref[SIDE * QUANTITIES * OWNED :, :] = jnp.where(
        row == 0, exp_ref[0], jnp.where(row == 1, exp_ref[1], exp_ref[2])
    )


def terms(k, order, weight, scale, exponent, masked, table):
    rows = SIDE * QUANTITIES * OWNED + 8
    smem = pl.BlockSpec(memory_space=pltpu.SMEM)

    def block(l):
        return pl.BlockSpec((DAYS, OWNED, WIDTH), lambda n, order: (0, order[4 * k + l], 0))

    return pl.pallas_call(
        terms_kernel,
        grid_spec=pltpu.PrefetchScalarGridSpec(
            num_scalar_prefetch=1,
            grid=(8,),
            in_specs=[smem, smem, smem]
            + [block(l) for l in range(SIDE)]
            + [pl.BlockSpec((WIDTH, 256), lambda n, order: (0, n))],
            out_specs=pl.BlockSpec((rows, 128), lambda n, order: (0, n)),
            scratch_shapes=[pltpu.VMEM((SIDE * DAYS * OWNED, WIDTH), jnp.bfloat16)],
        ),
        out_shape=jax.ShapeDtypeStruct((rows, WORDS), jnp.int32),
        compiler_params=params(dimension_semantics=("arbitrary",)),
        cost_estimate=pl.CostEstimate(
            flops=2 * SIDE * DAYS * OWNED * WIDTH * WIDTH, bytes_accessed=12 * MB, transcendentals=0
        ),
        name="terms",
    )(order, weight, scale, exponent, *([masked] * SIDE), table)


def read_sum(body_refs, exp_refs, q, cols):
    low = high = None
    for body, exp in zip(body_refs, exp_refs):
        k = unit(exp[q : q + 1, :])
        a, b = unpack(body[q * OWNED : (q + 1) * OWNED, cols])
        low = a * k if low is None else low + a * k
        high = b * k if high is None else high + b * k
    return low, high


def combine_kernel(*refs):
    body_refs, exp_refs, out_ref = refs[:SIDE], refs[SIDE : 2 * SIDE], refs[2 * SIDE]
    top = exp_refs[0][...]
    for exp in exp_refs[1:]:
        top = jnp.maximum(top, exp[...])
    top = top + 2
    scale = jnp.exp2(-0.5 * top.astype(jnp.float32)) * TOP
    for j in range(WORDS // 128):
        cols = slice(128 * j, 128 * j + 128)
        for q in range(QUANTITIES):
            low, high = read_sum(body_refs, exp_refs, q, cols)
            s = scale[q : q + 1, :]
            out_ref[q * OWNED : (q + 1) * OWNED, cols] = pack(encode(low, s), encode(high, s))
        out_ref[QUANTITIES * OWNED :, cols] = top


def combine(l, messages):
    body = pl.BlockSpec((QUANTITIES * OWNED, WORDS), lambda i: (l, 0))
    exps = pl.BlockSpec((8, 128), lambda i: (SIDE * QUANTITIES * OWNED // 8, 0))
    rows = QUANTITIES * OWNED + 8
    return pl.pallas_call(
        combine_kernel,
        grid=(1,),
        in_specs=[body] * SIDE + [exps] * SIDE,
        out_specs=pl.BlockSpec((rows, WORDS), lambda i: (0, 0)),
        out_shape=jax.ShapeDtypeStruct((rows, WORDS), jnp.int32),
        compiler_params=params(),
        cost_estimate=pl.CostEstimate(flops=2 * MB, bytes_accessed=2 * MB, transcendentals=0),
        name="combine",
    )(*messages, *messages)


def finish_kernel(divisor_ref, *refs):
    body_refs, exp_refs = refs[:SIDE], refs[SIDE : 2 * SIDE]
    weighted_ref, linear_ref = refs[2 * SIDE :]
    divisor = divisor_ref[...]
    for j in range(WORDS // 128):
        cols = slice(128 * j, 128 * j + 128)
        sums = [read_sum(body_refs, exp_refs, q, cols) for q in range(QUANTITIES)]
        for h in range(2):
            start = 128 * j + WORDS * h
            size = min(128, LAGS - start)
            linear = sums[0][h] / divisor
            real, imag = sums[1][h], sums[2][h]
            weighted = linear * ((real * real + imag * imag) / (divisor * divisor))
            linear_ref[:, start : start + size] = linear[:, :size]
            weighted_ref[:, start : start + size] = weighted[:, :size]


def finish(divisor, messages):
    body = pl.BlockSpec((QUANTITIES * OWNED, WORDS), lambda i: (0, 0))
    exps = pl.BlockSpec((8, 128), lambda i: (QUANTITIES * OWNED // 8, 0))
    out = pl.BlockSpec((OWNED, LAGS), lambda i: (0, 0))
    return pl.pallas_call(
        finish_kernel,
        grid=(1,),
        in_specs=[pl.BlockSpec((OWNED, 128), lambda i: (0, 0))] + [body] * SIDE + [exps] * SIDE,
        out_specs=[out, out],
        out_shape=[jax.ShapeDtypeStruct((OWNED, LAGS), jnp.float32)] * 2,
        compiler_params=params(),
        name="finish",
    )(divisor, *messages, *messages)


def shift(message, step, first):
    moves = []
    for x in range(SIDE):
        for y in range(SIDE):
            for pair in range(8):
                along_x = (pair % 2 == 0) == first
                to_x = (x + step) % SIDE if along_x else x
                to_y = y if along_x else (y + step) % SIDE
                moves.append(((x * SIDE + y) * 8 + pair, (to_x * SIDE + to_y) * 8 + pair))
    return lax.ppermute(message, ("day", "pair"), moves)


def exchange_small(values, axis):
    count = lax.axis_size(axis)
    return lax.all_to_all(jnp.broadcast_to(values[None], (count, *values.shape)), axis, 0, 0, tiled=True)


def stacks(correlations, mask, counts):
    masked = correlations * mask[:, :, None].astype(jnp.bfloat16)
    wide = masked.astype(jnp.float32)
    energy = jnp.sum(jnp.square(wide), axis=(1, 2))
    peak = jnp.max(jnp.abs(wide), axis=(1, 2))
    used_pairs = jnp.sum(mask, axis=1).astype(jnp.float32)
    totals = jnp.sum(exchange_small(jnp.concatenate([energy, used_pairs]), "pair"), axis=0)
    energy, used_pairs = totals[:DAYS], totals[DAYS:]
    weight = lax.rsqrt(energy / (LAGS * jnp.maximum(used_pairs, 1.0)) + 0.1)

    reach = weight * peak
    bounds = jnp.stack(
        [
            jnp.sum(reach),
            jnp.sum(jnp.minimum(1.0, 2.0 * reach)),
            jnp.sum(jnp.minimum(1.0, 2.0 * KERNEL_SUM * reach)),
        ]
    )
    exponent = jnp.ceil(jnp.log2(jnp.maximum(bounds, 1e-30) * 1.001)).astype(jnp.int32)
    scale = TOP * jnp.exp2(-0.5 * exponent.astype(jnp.float32))

    place = lax.axis_index("day")
    x, y = place // SIDE, place % SIDE
    core = lax.axis_index("pair") % 2
    a, b = jnp.arange(SIDE)[:, None], jnp.arange(SIDE)[None, :]
    order = jnp.where(
        core == 0,
        (x + a) % SIDE * SIDE + (y + b) % SIDE,
        (x + b) % SIDE * SIDE + (y + a) % SIDE,
    ).reshape(-1)

    table = kernel_table()

    def chunk(k):
        return terms(k, order, weight, scale, exponent, masked, table)

    def wide_step(k):
        piece = chunk(k)
        return shift(piece, k, True) if k else piece

    def narrow_step(l):
        piece = combine(l, messages)
        return shift(piece, l, False) if l else piece

    far, ahead, behind, own = [wide_step(k) for k in (2, 1, 3, 0)]
    messages = [own, ahead, far, behind]
    far, ahead, behind, own = [narrow_step(l) for l in (2, 1, 3, 0)]
    arrived = [own, ahead, far, behind]
    divisor = jnp.broadcast_to(jnp.maximum(counts.astype(jnp.float32), 1.0)[:, None], (OWNED, 128))
    return tuple(finish(divisor, arrived))


def solution(mesh):
    placed = (P("day", "pair", None), P("day", "pair"), P(("pair", "day")))
    return jax.shard_map(
        stacks,
        mesh=mesh,
        in_specs=placed,
        out_specs=(P(("pair", "day"), None), P(("pair", "day"), None)),
        check_vma=False,
    )
```

```python
import functools

import jax
import jax.numpy as jnp
from jax import lax
from jax.experimental import pallas as pl
from jax.experimental.pallas import tpu as pltpu
from jax.sharding import PartitionSpec as P


LAGS = 2001
WIDTH = 2048
WORDS = WIDTH // 2
OWNED = 32
DAYS = 4
SIDE = 4
QUANTITIES = 3
TOP = 32766.0
KERNEL_SUM = 6.0
MB = 1 << 20


def params(**settings):
    return pltpu.CompilerParams(**{"vmem_limit_bytes": 32 * MB, **settings})


def encode(value, scale):
    root = value * lax.rsqrt(jnp.abs(value) + 1e-36)
    return (root * scale + 32768.5).astype(jnp.int32)


def pack(low, high):
    return low | (high << 16)


def unpack(word):
    low = (word & 0xFFFF).astype(jnp.float32) - 32768.0
    high = (lax.shift_right_logical(word, 16)).astype(jnp.float32) - 32768.0
    return low * jnp.abs(low), high * jnp.abs(high)


def unit(exponent):
    return jnp.exp2(exponent.astype(jnp.float32)) * (1.0 / (TOP * TOP))


def first_shifts():
    row = lax.broadcasted_iota(jnp.int32, (8, 2 * WIDTH), 0)
    col = lax.broadcasted_iota(jnp.int32, (8, 2 * WIDTH), 1)
    offset = (col - row - WIDTH + 2 * LAGS) % LAGS
    offset = jnp.where(offset > LAGS // 2, offset - LAGS, offset)
    angle = jnp.pi * offset.astype(jnp.float32) / LAGS
    parity = 1.0 - 2.0 * (offset % 2).astype(jnp.float32)
    sine = jnp.where(offset == 0, 1.0, jnp.sin(angle))
    values = jnp.where(offset == 0, 0.0, (jnp.cos(angle) - parity) / (LAGS * sine))
    return values.astype(jnp.bfloat16).astype(jnp.float32)


def fill_table(shifts_ref, table_ref, rolled_ref):
    for q in range(16):
        first = pltpu.roll(shifts_ref[...], 16 * q, 1)
        second = pltpu.roll(shifts_ref[...], 16 * q + 8, 1)
        rolled_ref[16 * q : 16 * q + 16, :] = jnp.concatenate([first, second], 0).astype(jnp.bfloat16)
    for q in range(8):
        for n in range(8):
            for h in range(2):
                start = 128 * (n + 8 * h) - 256 * q + WIDTH
                table_ref[n, 256 * q : 256 * q + 256, 128 * h : 128 * h + 128] = rolled_ref[:, start : start + 128]


TILES = WIDTH // 128
GROUPS = 16


def position(owner, place):
    x, y, core = place >> 3, (place >> 1) & 3, place & 1
    along_x, along_y = (owner // SIDE - x) & 3, (owner % SIDE - y) & 3
    return jnp.where(core == 0, along_x * SIDE + along_y, along_y * SIDE + along_x)


def rows_kernel(
    place_ref, input_ref, mask_ref, shifts_ref, out_ref, table_ref, stats_ref, peak_ref, *scratch
):
    held_ref, square_ref, most_ref, rolled_ref, sems = scratch
    place = place_ref[0]
    last = (LAGS - 128 * (TILES - 1)) * GROUPS

    def fetch(j, size):
        return pltpu.make_async_copy(
            input_ref.at[pl.ds(j * 128 * GROUPS, size), :], held_ref.at[j, pl.ds(0, size), :], sems.at[j]
        )

    for j in range(TILES):
        fetch(j, 128 * GROUPS if j < TILES - 1 else last).start()
    fill_table(shifts_ref, table_ref, rolled_ref)
    held_ref[TILES - 1, last:, :] = jnp.zeros((128 * GROUPS - last, 128), jnp.bfloat16)
    square_ref[...] = jnp.zeros_like(square_ref)
    most_ref[...] = jnp.zeros_like(most_ref)
    row = lax.broadcasted_iota(jnp.int32, (256, 256), 0)
    col = lax.broadcasted_iota(jnp.int32, (256, 256), 1)
    select = ((row // 16 == col % 16) & (row % 16 == col // 16)).astype(jnp.float32).astype(jnp.bfloat16)
    places = [position(owner, place) for owner in range(SIDE * SIDE)]

    def tile(j):
        parts = []
        for b in range(4):
            first = held_ref[j, 512 * b : 512 * b + 256, :]
            second = held_ref[j, 512 * b + 256 : 512 * b + 512, :]
            parts.append(
                jnp.dot(select, jnp.concatenate([first, second], 1), preferred_element_type=jnp.float32)
            )
        for t in range(4):
            for d in range(DAYS):
                at = 16 * (t * DAYS + d)
                pieces = [p[at : at + 16, 128 * h : 128 * h + 128] for p in parts for h in range(2)]
                used = mask_ref[d : d + 1, 128 * t : 128 * t + 128].astype(jnp.float32)
                values = jnp.concatenate(pieces, 0) * used
                squares = (values * values).reshape(16, 8, 128)
                square_ref[d] += jnp.sum(squares, axis=0)
                most_ref[d] = jnp.maximum(most_ref[d], jnp.max(squares, axis=0))
                turned = values.T.astype(jnp.bfloat16)
                for i in range(4):
                    lanes = pl.ds(pl.multiple_of(j * 128, 128), 128)
                    out_ref[places[t * 4 + i], d, :, lanes] = turned[OWNED * i : OWNED * i + OWNED, :]

    def step(j, carry):
        fetch(j, 128 * GROUPS).wait()
        tile(j)
        return carry

    lax.fori_loop(0, TILES - 1, step, 0)
    fetch(TILES - 1, last).wait()
    tile(TILES - 1)

    row = lax.broadcasted_iota(jnp.int32, (8, 128), 0)
    stats = peaks = jnp.zeros((8, 128), jnp.float32)
    for d in range(DAYS):
        stats = jnp.where(row == d, jnp.sum(square_ref[d]), stats)
        stats = jnp.where(row == DAYS + d, jnp.sum(mask_ref[d : d + 1, :].astype(jnp.float32)), stats)
        peaks = jnp.where(row == d, jnp.max(most_ref[d]), peaks)
    peak_ref[...] = peaks
    for i in range(8):
        stats_ref[i] = stats


def ordered_rows(place, correlations, mask):
    stored = correlations.reshape(DAYS, 4, 128, LAGS).transpose(3, 1, 0, 2).reshape(LAGS * GROUPS, 128)
    vmem = pl.BlockSpec(memory_space=pltpu.VMEM)
    return pl.pallas_call(
        rows_kernel,
        in_specs=[
            pl.BlockSpec(memory_space=pltpu.SMEM),
            pl.BlockSpec(memory_space=pltpu.HBM),
            vmem,
            vmem,
        ],
        out_specs=[vmem] * 4,
        out_shape=[
            jax.ShapeDtypeStruct((SIDE * SIDE, DAYS, OWNED, WIDTH), jnp.bfloat16),
            jax.ShapeDtypeStruct((8, WIDTH, 256), jnp.bfloat16),
            jax.ShapeDtypeStruct((8, 8, 128), jnp.float32),
            jax.ShapeDtypeStruct((8, 128), jnp.float32),
        ],
        scratch_shapes=[
            pltpu.VMEM((TILES, 128 * GROUPS, 128), jnp.bfloat16),
            pltpu.VMEM((DAYS, 8, 128), jnp.float32),
            pltpu.VMEM((DAYS, 8, 128), jnp.float32),
            pltpu.VMEM((256, 2 * WIDTH), jnp.bfloat16),
            pltpu.SemaphoreType.DMA((TILES,)),
        ],
        compiler_params=params(vmem_limit_bytes=28 * MB),
        name="rows",
    )(place, pltpu.with_memory_space_constraint(stored, pltpu.HBM), mask, first_shifts())


def terms_kernel(k, rows_ref, table_ref, stats_ref, peak_ref, out_ref, even_ref, odd_ref):
    total = jnp.sum(stats_ref[...], axis=0)
    energy, used = total[:DAYS, :], total[DAYS:, :]
    weight = lax.rsqrt(energy / (LAGS * jnp.maximum(used, 1.0)) + 0.1)
    reach = weight * jnp.sqrt(peak_ref[:DAYS, :])
    bounds = [
        jnp.sum(reach, axis=0, keepdims=True),
        jnp.sum(jnp.minimum(1.0, 2.0 * reach), axis=0, keepdims=True),
        jnp.sum(jnp.minimum(1.0, 2.0 * KERNEL_SUM * reach), axis=0, keepdims=True),
    ]
    powers = [jnp.ceil(jnp.log(jnp.maximum(v, 1e-30) * 1.001) * 1.4426951) for v in bounds]
    scale = [TOP * jnp.exp2(-0.5 * p) for p in powers]
    row = lax.broadcasted_iota(jnp.int32, (8, 128), 0)
    exponents = jnp.where(row == 0, powers[0], jnp.where(row == 1, powers[1], powers[2])).astype(jnp.int32)
    for n in range(WORDS // 128):
        out_ref[SIDE * QUANTITIES * OWNED :, 128 * n : 128 * n + 128] = exponents
    weights = [weight[d : d + 1, :] for d in range(DAYS)]

    def product(n, to_ref):
        to_ref[...] = jnp.dot(rows_ref[k], table_ref[n], preferred_element_type=jnp.float32)

    def finish_block(n, hilbert_ref):
        for l in range(SIDE):
            codes = []
            for h in range(2):
                lanes = pl.ds(pl.multiple_of(n * 128 + h * WORDS, 128), 128)
                linear = real = imag = None
                for d in range(DAYS):
                    at = (l * DAYS + d) * OWNED
                    real_part = rows_ref[k, at : at + OWNED, lanes].astype(jnp.float32) * weights[d]
                    imag_part = hilbert_ref[at : at + OWNED, 128 * h : 128 * h + 128] * weights[d]
                    inverse = lax.rsqrt(real_part * real_part + imag_part * imag_part + 0.25)
                    a, b = real_part * inverse, imag_part * inverse
                    linear = real_part if d == 0 else linear + real_part
                    real = a if d == 0 else real + a
                    imag = b if d == 0 else imag + b
                codes.append([encode(v, scale[q]) for q, v in enumerate((linear, real, imag))])
            for q in range(QUANTITIES):
                at = (l * QUANTITIES + q) * OWNED
                out_ref[at : at + OWNED, pl.ds(pl.multiple_of(n * 128, 128), 128)] = pack(codes[0][q], codes[1][q])

    def step(i, carry):
        product(2 * i + 1, odd_ref)
        finish_block(2 * i, even_ref)
        product(2 * i + 2, even_ref)
        finish_block(2 * i + 1, odd_ref)
        return carry

    product(0, even_ref)
    lax.fori_loop(0, 3, step, 0)
    product(7, odd_ref)
    finish_block(6, even_ref)
    finish_block(7, odd_ref)


def terms(k, rows, table, stats, peak):
    count = SIDE * QUANTITIES * OWNED + 8
    vmem = pl.BlockSpec(memory_space=pltpu.VMEM)
    return pl.pallas_call(
        functools.partial(terms_kernel, k),
        in_specs=[vmem] * 4,
        out_specs=vmem,
        out_shape=jax.ShapeDtypeStruct((count, WORDS), jnp.int32),
        scratch_shapes=[pltpu.VMEM((SIDE * DAYS * OWNED, 256), jnp.float32)] * 2,
        compiler_params=params(vmem_limit_bytes=24 * MB),
        cost_estimate=pl.CostEstimate(
            flops=2 * SIDE * DAYS * OWNED * WIDTH * WIDTH, bytes_accessed=12 * MB, transcendentals=0
        ),
        name="terms",
    )(rows, table, stats, peak)


def read_sum(body_refs, exp_refs, q, cols):
    low = high = None
    for body, exp in zip(body_refs, exp_refs):
        k = unit(exp[q : q + 1, :])
        a, b = unpack(body[q * OWNED : (q + 1) * OWNED, cols])
        low = a * k if low is None else low + a * k
        high = b * k if high is None else high + b * k
    return low, high


def combine_kernel(*refs):
    body_refs, exp_refs, out_ref = refs[:SIDE], refs[SIDE : 2 * SIDE], refs[2 * SIDE]
    top = exp_refs[0][...]
    for exp in exp_refs[1:]:
        top = jnp.maximum(top, exp[...])
    top = top + 2
    scale = jnp.exp2(-0.5 * top.astype(jnp.float32)) * TOP
    for j in range(WORDS // 128):
        cols = slice(128 * j, 128 * j + 128)
        for q in range(QUANTITIES):
            low, high = read_sum(body_refs, exp_refs, q, cols)
            s = scale[q : q + 1, :]
            out_ref[q * OWNED : (q + 1) * OWNED, cols] = pack(encode(low, s), encode(high, s))
        out_ref[QUANTITIES * OWNED :, cols] = top


def combine(l, messages):
    body = pl.BlockSpec((QUANTITIES * OWNED, WORDS), lambda i: (l, 0))
    exps = pl.BlockSpec((8, 128), lambda i: (SIDE * QUANTITIES * OWNED // 8, 0))
    rows = QUANTITIES * OWNED + 8
    return pl.pallas_call(
        combine_kernel,
        grid=(1,),
        in_specs=[body] * SIDE + [exps] * SIDE,
        out_specs=pl.BlockSpec((rows, WORDS), lambda i: (0, 0)),
        out_shape=jax.ShapeDtypeStruct((rows, WORDS), jnp.int32),
        compiler_params=params(),
        cost_estimate=pl.CostEstimate(flops=2 * MB, bytes_accessed=2 * MB, transcendentals=0),
        name="combine",
    )(*messages, *messages)


def finish_kernel(divisor_ref, *refs):
    body_refs, exp_refs = refs[:SIDE], refs[SIDE : 2 * SIDE]
    weighted_ref, linear_ref = refs[2 * SIDE :]
    divisor = divisor_ref[...]
    for j in range(WORDS // 128):
        cols = slice(128 * j, 128 * j + 128)
        sums = [read_sum(body_refs, exp_refs, q, cols) for q in range(QUANTITIES)]
        for h in range(2):
            start = 128 * j + WORDS * h
            size = min(128, LAGS - start)
            linear = sums[0][h] / divisor
            real, imag = sums[1][h], sums[2][h]
            weighted = linear * ((real * real + imag * imag) / (divisor * divisor))
            linear_ref[:, start : start + size] = linear[:, :size]
            weighted_ref[:, start : start + size] = weighted[:, :size]


def finish(divisor, messages):
    body = pl.BlockSpec((QUANTITIES * OWNED, WORDS), lambda i: (0, 0))
    exps = pl.BlockSpec((8, 128), lambda i: (QUANTITIES * OWNED // 8, 0))
    out = pl.BlockSpec((OWNED, LAGS), lambda i: (0, 0))
    return pl.pallas_call(
        finish_kernel,
        grid=(1,),
        in_specs=[pl.BlockSpec((OWNED, 128), lambda i: (0, 0))] + [body] * SIDE + [exps] * SIDE,
        out_specs=[out, out],
        out_shape=[jax.ShapeDtypeStruct((OWNED, LAGS), jnp.float32)] * 2,
        compiler_params=params(),
        name="finish",
    )(divisor, *messages, *messages)


def shift(message, step, first):
    moves = []
    for x in range(SIDE):
        for y in range(SIDE):
            for pair in range(8):
                along_x = (pair % 2 == 0) == first
                to_x = (x + step) % SIDE if along_x else x
                to_y = y if along_x else (y + step) % SIDE
                moves.append(((x * SIDE + y) * 8 + pair, (to_x * SIDE + to_y) * 8 + pair))
    return lax.ppermute(message, ("day", "pair"), moves)


def stacks(correlations, mask, counts):
    place = (lax.axis_index("day") * 2 + lax.axis_index("pair") % 2).reshape(1)
    rows, table, stats, peak = ordered_rows(place, correlations, mask)
    rows = rows.reshape(SIDE, SIDE * DAYS * OWNED, WIDTH)
    stats = lax.all_to_all(stats, "pair", 0, 0, tiled=True)

    def wide_step(k):
        piece = terms(k, rows, table, stats, peak)
        return shift(piece, k, True) if k else piece

    def narrow_step(l):
        piece = combine(l, messages)
        return shift(piece, l, False) if l else piece

    far, ahead, behind, own = [wide_step(k) for k in (2, 1, 3, 0)]
    messages = [own, ahead, far, behind]
    far, ahead, behind, own = [narrow_step(l) for l in (2, 1, 3, 0)]
    arrived = [own, ahead, far, behind]
    divisor = jnp.broadcast_to(jnp.maximum(counts.astype(jnp.float32), 1.0)[:, None], (OWNED, 128))
    return tuple(finish(divisor, arrived))


def solution(mesh):
    placed = (P("day", "pair", None), P("day", "pair"), P(("pair", "day")))
    return jax.shard_map(
        stacks,
        mesh=mesh,
        in_specs=placed,
        out_specs=(P(("pair", "day"), None), P(("pair", "day"), None)),
        check_vma=False,
    )
```

```python
import functools

import jax
import jax.numpy as jnp
from jax import lax
from jax.experimental import pallas as pl
from jax.experimental.pallas import tpu as pltpu
from jax.sharding import PartitionSpec as P


LAGS = 2001
WIDTH = 2048
WORDS = WIDTH // 2
OWNED = 32
DAYS = 4
SIDE = 4
QUANTITIES = 3
TOP = 32766.0
KERNEL_SUM = 6.0
MB = 1 << 20


def params(**settings):
    return pltpu.CompilerParams(**{"vmem_limit_bytes": 32 * MB, **settings})


def encode(value, scale):
    root = value * lax.rsqrt(jnp.abs(value) + 1e-36)
    return (root * scale + 32768.5).astype(jnp.int32)


def pack(low, high):
    return low | (high << 16)


def unpack(word):
    low = (word & 0xFFFF).astype(jnp.float32) - 32768.0
    high = (lax.shift_right_logical(word, 16)).astype(jnp.float32) - 32768.0
    return low * jnp.abs(low), high * jnp.abs(high)


def unit(exponent):
    return jnp.exp2(exponent.astype(jnp.float32)) * (1.0 / (TOP * TOP))


def first_shifts():
    row = lax.broadcasted_iota(jnp.int32, (8, 2 * WIDTH), 0)
    col = lax.broadcasted_iota(jnp.int32, (8, 2 * WIDTH), 1)
    offset = (col - row - WIDTH + 2 * LAGS) % LAGS
    offset = jnp.where(offset > LAGS // 2, offset - LAGS, offset)
    angle = jnp.pi * offset.astype(jnp.float32) / LAGS
    parity = 1.0 - 2.0 * (offset % 2).astype(jnp.float32)
    sine = jnp.where(offset == 0, 1.0, jnp.sin(angle))
    values = jnp.where(offset == 0, 0.0, (jnp.cos(angle) - parity) / (LAGS * sine))
    return values.astype(jnp.bfloat16).astype(jnp.float32)


def fill_table(shifts_ref, table_ref, rolled_ref):
    for q in range(16):
        first = pltpu.roll(shifts_ref[...], 16 * q, 1)
        second = pltpu.roll(shifts_ref[...], 16 * q + 8, 1)
        rolled_ref[16 * q : 16 * q + 16, :] = jnp.concatenate([first, second], 0).astype(jnp.bfloat16)
    for q in range(8):
        for n in range(8):
            for h in range(2):
                start = 128 * (n + 8 * h) - 256 * q + WIDTH
                table_ref[n, 256 * q : 256 * q + 256, 128 * h : 128 * h + 128] = rolled_ref[:, start : start + 128]


TILES = WIDTH // 128
GROUPS = 16


def position(owner, place):
    x, y, core = place >> 3, (place >> 1) & 3, place & 1
    along_x, along_y = (owner // SIDE - x) & 3, (owner % SIDE - y) & 3
    return jnp.where(core == 0, along_x * SIDE + along_y, along_y * SIDE + along_x)


def energy_kernel(place_ref, input_ref, mask_ref, shifts_ref, held_ref, stats_ref, peak_ref, sems):
    last = (LAGS - 128 * (TILES - 1)) * GROUPS

    def fetch(j, size):
        return pltpu.make_async_copy(
            input_ref.at[pl.ds(j * 128 * GROUPS, size), :], held_ref.at[j, pl.ds(0, size), :], sems.at[j]
        )

    for j in range(TILES):
        fetch(j, 128 * GROUPS if j < TILES - 1 else last).start()
    held_ref[TILES - 1, last:, :] = jnp.zeros((128 * GROUPS - last, 128), jnp.bfloat16)
    used = jnp.concatenate([mask_ref[:, 128 * t : 128 * t + 128] for t in range(4)], 0).astype(jnp.float32)

    def tile(j, carry):
        total, most = carry
        for b in range(8):
            values = held_ref[j, 256 * b : 256 * b + 256, :].astype(jnp.float32)
            squares = (values * values).reshape(16, GROUPS, 128)
            total += jnp.sum(squares, axis=0)
            most = jnp.maximum(most, jnp.max(squares, axis=0))
        return total, most

    def step(j, carry):
        fetch(j, 128 * GROUPS).wait()
        return tile(j, carry)

    zero = jnp.zeros((GROUPS, 128), jnp.float32)
    carry = lax.fori_loop(0, TILES - 1, step, (zero, zero))
    fetch(TILES - 1, last).wait()
    total, most = tile(TILES - 1, carry)
    total, most = total * used, most * used

    row = lax.broadcasted_iota(jnp.int32, (8, 128), 0)
    day = lax.broadcasted_iota(jnp.int32, (GROUPS, 128), 0) % DAYS
    stats = peaks = jnp.zeros((8, 128), jnp.float32)
    for d in range(DAYS):
        stats = jnp.where(row == d, jnp.sum(jnp.where(day == d, total, 0.0)), stats)
        stats = jnp.where(row == DAYS + d, jnp.sum(jnp.where(day == d, used, 0.0)), stats)
        peaks = jnp.where(row == d, jnp.max(jnp.where(day == d, most, 0.0)), peaks)
    peak_ref[...] = peaks
    stats_ref[...] = stats


def energies(place, correlations, mask, shifts):
    stored = correlations.reshape(DAYS, 4, 128, LAGS).transpose(3, 1, 0, 2).reshape(LAGS * GROUPS, 128)
    vmem = pl.BlockSpec(memory_space=pltpu.VMEM)
    return pl.pallas_call(
        energy_kernel,
        in_specs=[pl.BlockSpec(memory_space=pltpu.SMEM), pl.BlockSpec(memory_space=pltpu.HBM), vmem, vmem],
        out_specs=[vmem] * 3,
        out_shape=[
            jax.ShapeDtypeStruct((TILES, 128 * GROUPS, 128), jnp.bfloat16),
            jax.ShapeDtypeStruct((8, 128), jnp.float32),
            jax.ShapeDtypeStruct((8, 128), jnp.float32),
        ],
        scratch_shapes=[pltpu.SemaphoreType.DMA((TILES,))],
        compiler_params=params(vmem_limit_bytes=12 * MB),
        name="energy",
    )(place, pltpu.with_memory_space_constraint(stored, pltpu.HBM), mask, shifts)


def rows_kernel(first_tile, last_tile, place_ref, held_ref, mask_ref, *refs):
    out_ref = refs[-1]
    place = place_ref[0]
    row = lax.broadcasted_iota(jnp.int32, (256, 256), 0)
    col = lax.broadcasted_iota(jnp.int32, (256, 256), 1)
    select = ((row // 16 == col % 16) & (row % 16 == col // 16)).astype(jnp.float32).astype(jnp.bfloat16)
    places = [position(owner, place) for owner in range(SIDE * SIDE)]

    def tile(j, carry):
        parts = []
        for b in range(4):
            first = held_ref[j, 512 * b : 512 * b + 256, :]
            second = held_ref[j, 512 * b + 256 : 512 * b + 512, :]
            parts.append(
                jnp.dot(select, jnp.concatenate([first, second], 1), preferred_element_type=jnp.float32)
            )
        for t in range(4):
            for d in range(DAYS):
                at = 16 * (t * DAYS + d)
                pieces = [p[at : at + 16, 128 * h : 128 * h + 128] for p in parts for h in range(2)]
                used = mask_ref[d : d + 1, 128 * t : 128 * t + 128].astype(jnp.float32)
                turned = (jnp.concatenate(pieces, 0) * used).astype(jnp.bfloat16).T
                for i in range(4):
                    lanes = pl.ds(pl.multiple_of(j * 128, 128), 128)
                    out_ref[places[t * 4 + i], d, :, lanes] = turned[OWNED * i : OWNED * i + OWNED, :]
        return carry

    lax.fori_loop(first_tile, last_tile, tile, 0)


def ordered_rows(place, held, mask, before=None):
    vmem = pl.BlockSpec(memory_space=pltpu.VMEM)
    tiles = (0, TILES // 2) if before is None else (TILES // 2, TILES)
    started = [] if before is None else [before]
    return pl.pallas_call(
        functools.partial(rows_kernel, *tiles),
        in_specs=[pl.BlockSpec(memory_space=pltpu.SMEM)] + [vmem] * (2 + len(started)),
        out_specs=vmem,
        out_shape=jax.ShapeDtypeStruct((SIDE * SIDE, DAYS, OWNED, WIDTH), jnp.bfloat16),
        input_output_aliases={3: 0} if started else {},
        compiler_params=params(vmem_limit_bytes=12 * MB),
        cost_estimate=pl.CostEstimate(flops=4 * 10**9, bytes_accessed=8 * MB, transcendentals=0),
        name="rows",
    )(place, held, mask, *started)


def kernel_table(shifts):
    vmem = pl.BlockSpec(memory_space=pltpu.VMEM)
    return pl.pallas_call(
        fill_table,
        in_specs=[vmem],
        out_specs=vmem,
        out_shape=jax.ShapeDtypeStruct((8, WIDTH, 256), jnp.bfloat16),
        scratch_shapes=[pltpu.VMEM((256, 2 * WIDTH), jnp.bfloat16)],
        compiler_params=params(vmem_limit_bytes=12 * MB),
        cost_estimate=pl.CostEstimate(flops=10**9, bytes_accessed=8 * MB, transcendentals=0),
        name="table",
    )(shifts)


def add_kernel(a_ref, b_ref, out_ref):
    out_ref[...] = a_ref[...] + b_ref[...]


def add(a, b):
    vmem = pl.BlockSpec(memory_space=pltpu.VMEM)
    return pl.pallas_call(
        add_kernel,
        in_specs=[vmem] * 2,
        out_specs=vmem,
        out_shape=jax.ShapeDtypeStruct(a.shape, a.dtype),
        compiler_params=params(vmem_limit_bytes=MB),
        name="add",
    )(a, b)


def terms_kernel(k, rows_ref, table_ref, stats_ref, others_ref, peak_ref, out_ref, even_ref, odd_ref):
    total = stats_ref[...] + others_ref[...]
    energy, used = total[:DAYS, :], total[DAYS:, :]
    weight = lax.rsqrt(energy / (LAGS * jnp.maximum(used, 1.0)) + 0.1)
    reach = weight * jnp.sqrt(peak_ref[:DAYS, :])
    bounds = [
        jnp.sum(reach, axis=0, keepdims=True),
        jnp.sum(jnp.minimum(1.0, 2.0 * reach), axis=0, keepdims=True),
        jnp.sum(jnp.minimum(1.0, 2.0 * KERNEL_SUM * reach), axis=0, keepdims=True),
    ]
    powers = [jnp.ceil(jnp.log(jnp.maximum(v, 1e-30) * 1.001) * 1.4426951) for v in bounds]
    scale = [TOP * jnp.exp2(-0.5 * p) for p in powers]
    row = lax.broadcasted_iota(jnp.int32, (8, 128), 0)
    exponents = jnp.where(row == 0, powers[0], jnp.where(row == 1, powers[1], powers[2])).astype(jnp.int32)
    for n in range(WORDS // 128):
        out_ref[SIDE * QUANTITIES * OWNED :, 128 * n : 128 * n + 128] = exponents
    weights = [weight[d : d + 1, :] for d in range(DAYS)]

    def product(n, to_ref):
        to_ref[...] = jnp.dot(rows_ref[k], table_ref[n], preferred_element_type=jnp.float32)

    def finish_block(n, hilbert_ref):
        for l in range(SIDE):
            codes = []
            for h in range(2):
                lanes = pl.ds(pl.multiple_of(n * 128 + h * WORDS, 128), 128)
                linear = real = imag = None
                for d in range(DAYS):
                    at = (l * DAYS + d) * OWNED
                    real_part = rows_ref[k, at : at + OWNED, lanes].astype(jnp.float32) * weights[d]
                    imag_part = hilbert_ref[at : at + OWNED, 128 * h : 128 * h + 128] * weights[d]
                    inverse = lax.rsqrt(real_part * real_part + imag_part * imag_part + 0.25)
                    a, b = real_part * inverse, imag_part * inverse
                    linear = real_part if d == 0 else linear + real_part
                    real = a if d == 0 else real + a
                    imag = b if d == 0 else imag + b
                codes.append([encode(v, scale[q]) for q, v in enumerate((linear, real, imag))])
            for q in range(QUANTITIES):
                at = (l * QUANTITIES + q) * OWNED
                out_ref[at : at + OWNED, pl.ds(pl.multiple_of(n * 128, 128), 128)] = pack(codes[0][q], codes[1][q])

    def step(i, carry):
        product(2 * i + 1, odd_ref)
        finish_block(2 * i, even_ref)
        product(2 * i + 2, even_ref)
        finish_block(2 * i + 1, odd_ref)
        return carry

    product(0, even_ref)
    lax.fori_loop(0, 3, step, 0)
    product(7, odd_ref)
    finish_block(6, even_ref)
    finish_block(7, odd_ref)


def terms(k, rows, table, *stats):
    count = SIDE * QUANTITIES * OWNED + 8
    vmem = pl.BlockSpec(memory_space=pltpu.VMEM)
    return pl.pallas_call(
        functools.partial(terms_kernel, k),
        in_specs=[vmem] * 5,
        out_specs=vmem,
        out_shape=jax.ShapeDtypeStruct((count, WORDS), jnp.int32),
        scratch_shapes=[pltpu.VMEM((SIDE * DAYS * OWNED, 256), jnp.float32)] * 2,
        compiler_params=params(vmem_limit_bytes=24 * MB),
        cost_estimate=pl.CostEstimate(
            flops=2 * SIDE * DAYS * OWNED * WIDTH * WIDTH, bytes_accessed=12 * MB, transcendentals=0
        ),
        name="terms",
    )(rows, table, *stats)


def decode(message_ref, at, exponent, cols):
    k = unit(exponent)
    low, high = unpack(message_ref[at : at + OWNED, cols])
    return low * k, high * k


def gather_kernel(parts, blocks, *refs):
    messages, (out_ref, top_ref) = refs[:parts], refs[parts:]
    rows = blocks * QUANTITIES * OWNED
    top = messages[0][rows : rows + 8, :128]
    for message in messages[1:]:
        top = jnp.maximum(top, message[rows : rows + 8, :128])
    top_ref[...] = top
    for l in range(blocks):
        for j in range(WORDS // 128):
            cols = slice(128 * j, 128 * j + 128)
            for q in range(QUANTITIES):
                at = (l * QUANTITIES + q) * OWNED
                low = high = None
                for message in messages:
                    a, b = decode(message, at, message[rows + q : rows + q + 1, :128], cols)
                    low = a if low is None else low + a
                    high = b if high is None else high + b
                out_ref[at : at + OWNED, cols] = low
                out_ref[at : at + OWNED, 128 * j + WORDS : 128 * j + WORDS + 128] = high


def gather(messages, blocks):
    vmem = pl.BlockSpec(memory_space=pltpu.VMEM)
    return pl.pallas_call(
        functools.partial(gather_kernel, len(messages), blocks),
        in_specs=[vmem] * len(messages),
        out_specs=[vmem] * 2,
        out_shape=[
            jax.ShapeDtypeStruct((blocks * QUANTITIES * OWNED, WIDTH), jnp.float32),
            jax.ShapeDtypeStruct((8, 128), jnp.int32),
        ],
        compiler_params=params(vmem_limit_bytes=16 * MB),
        cost_estimate=pl.CostEstimate(flops=blocks * MB, bytes_accessed=2 * MB, transcendentals=0),
        name="gather",
    )(*messages)


def combine_kernel(l, sums_ref, top_ref, *refs):
    messages, out_ref = refs[:-1], refs[-1]
    rows = SIDE * QUANTITIES * OWNED
    exponents = [message[rows : rows + 8, :128] for message in messages]
    top = top_ref[...]
    for exponent in exponents:
        top = jnp.maximum(top, exponent)
    top = top + 2
    scale = jnp.exp2(-0.5 * top.astype(jnp.float32)) * TOP
    for j in range(WORDS // 128):
        cols = slice(128 * j, 128 * j + 128)
        for q in range(QUANTITIES):
            at = (l * QUANTITIES + q) * OWNED
            low = sums_ref[at : at + OWNED, cols]
            high = sums_ref[at : at + OWNED, 128 * j + WORDS : 128 * j + WORDS + 128]
            for message, exponent in zip(messages, exponents):
                a, b = decode(message, at, exponent[q : q + 1, :], cols)
                low, high = low + a, high + b
            s = scale[q : q + 1, :]
            out_ref[q * OWNED : (q + 1) * OWNED, cols] = pack(encode(low, s), encode(high, s))
        out_ref[QUANTITIES * OWNED :, cols] = top


def combine(l, sums, top, messages):
    vmem = pl.BlockSpec(memory_space=pltpu.VMEM)
    return pl.pallas_call(
        functools.partial(combine_kernel, l),
        in_specs=[vmem] * (2 + len(messages)),
        out_specs=vmem,
        out_shape=jax.ShapeDtypeStruct((QUANTITIES * OWNED + 8, WORDS), jnp.int32),
        compiler_params=params(vmem_limit_bytes=16 * MB),
        cost_estimate=pl.CostEstimate(flops=2 * MB, bytes_accessed=2 * MB, transcendentals=0),
        name="combine",
    )(sums, top, *messages)


def finish_kernel(divisor_ref, sums_ref, message_ref, weighted_ref, linear_ref):
    inverse = 1.0 / divisor_ref[...]
    rows = QUANTITIES * OWNED
    exponents = message_ref[rows : rows + 8, :128]
    for j in range(WORDS // 128):
        cols = slice(128 * j, 128 * j + 128)
        pairs = [decode(message_ref, q * OWNED, exponents[q : q + 1, :], cols) for q in range(QUANTITIES)]
        for h in range(2):
            start = 128 * j + WORDS * h
            size = min(128, LAGS - start)
            linear, real, imag = [
                pairs[q][h] + sums_ref[q * OWNED : (q + 1) * OWNED, start : start + 128] for q in range(QUANTITIES)
            ]
            linear, real, imag = linear * inverse, real * inverse, imag * inverse
            weighted = linear * (real * real + imag * imag)
            linear_ref[:, start : start + size] = linear[:, :size]
            weighted_ref[:, start : start + size] = weighted[:, :size]


def finish(divisor, sums, message):
    vmem = pl.BlockSpec(memory_space=pltpu.VMEM)
    return pl.pallas_call(
        finish_kernel,
        in_specs=[vmem] * 3,
        out_specs=[vmem] * 2,
        out_shape=[jax.ShapeDtypeStruct((OWNED, LAGS), jnp.float32)] * 2,
        compiler_params=params(vmem_limit_bytes=16 * MB),
        name="finish",
    )(divisor, sums, message)


def shift(message, step, first):
    moves = []
    for x in range(SIDE):
        for y in range(SIDE):
            for pair in range(8):
                along_x = (pair % 2 == 0) == first
                to_x = (x + step) % SIDE if along_x else x
                to_y = y if along_x else (y + step) % SIDE
                moves.append(((x * SIDE + y) * 8 + pair, (to_x * SIDE + to_y) * 8 + pair))
    return lax.ppermute(message, ("day", "pair"), moves)


def trade(values, bit):
    moves = [(d * 8 + p, d * 8 + (p ^ bit)) for d in range(SIDE * SIDE) for p in range(8)]
    return lax.ppermute(values, ("day", "pair"), moves)


def stacks(correlations, mask, counts):
    place = (lax.axis_index("day") * 2 + lax.axis_index("pair") % 2).reshape(1)
    shifts = first_shifts()
    held, stats, peak = energies(place, correlations, mask, shifts)
    others = trade(stats, 1)
    table = kernel_table(shifts)
    stats = add(stats, others)
    others = trade(stats, 2)
    rows = ordered_rows(place, held, mask)
    stats = add(stats, others)
    others = trade(stats, 4)
    rows = ordered_rows(place, held, mask, rows)
    rows = rows.reshape(SIDE, SIDE * DAYS * OWNED, WIDTH)

    def wide_step(k):
        piece = terms(k, rows, table, stats, others, peak)
        return shift(piece, k, True) if k else piece

    def narrow_step(l):
        piece = combine(l, sums, top, [ahead, behind])
        return shift(piece, l, False) if l else piece

    far, ahead, behind, own = [wide_step(k) for k in (2, 1, 3, 0)]
    sums, top = gather([own, far], SIDE)
    last, near, far, own = [narrow_step(l) for l in (2, 1, 3, 0)]
    sums, top = gather([own, near, far], 1)
    divisor = jnp.broadcast_to(jnp.maximum(counts.astype(jnp.float32), 1.0)[:, None], (OWNED, 128))
    return tuple(finish(divisor, sums, last))


def solution(mesh):
    placed = (P("day", "pair", None), P("day", "pair"), P(("pair", "day")))
    return jax.shard_map(
        stacks,
        mesh=mesh,
        in_specs=placed,
        out_specs=(P(("pair", "day"), None), P(("pair", "day"), None)),
        check_vma=False,
    )
```

```python
import functools

import jax
import jax.numpy as jnp
from jax import lax
from jax.experimental import pallas as pl
from jax.experimental.pallas import tpu as pltpu
from jax.sharding import PartitionSpec as P


LAGS = 2001
WIDTH = 2048
WORDS = WIDTH // 2
OWNED = 32
DAYS = 4
SIDE = 4
QUANTITIES = 3
TOP = 32766.0
KERNEL_SUM = 6.0
MB = 1 << 20


def params(**settings):
    return pltpu.CompilerParams(**{"vmem_limit_bytes": 32 * MB, **settings})


def encode(value, scale):
    root = value * lax.rsqrt(jnp.abs(value) + 1e-36)
    return (root * scale + 32768.5).astype(jnp.int32)


def pack(low, high):
    return low | (high << 16)


def unpack(word):
    low = (word & 0xFFFF).astype(jnp.float32) - 32768.0
    high = (lax.shift_right_logical(word, 16)).astype(jnp.float32) - 32768.0
    return low * jnp.abs(low), high * jnp.abs(high)


def unit(exponent):
    return jnp.exp2(exponent.astype(jnp.float32)) * (1.0 / (TOP * TOP))


def first_shifts():
    row = lax.broadcasted_iota(jnp.int32, (8, 2 * WIDTH), 0)
    col = lax.broadcasted_iota(jnp.int32, (8, 2 * WIDTH), 1)
    offset = (col - row - WIDTH + 2 * LAGS) % LAGS
    offset = jnp.where(offset > LAGS // 2, offset - LAGS, offset)
    angle = jnp.pi * offset.astype(jnp.float32) / LAGS
    parity = 1.0 - 2.0 * (offset % 2).astype(jnp.float32)
    sine = jnp.where(offset == 0, 1.0, jnp.sin(angle))
    values = jnp.where(offset == 0, 0.0, (jnp.cos(angle) - parity) / (LAGS * sine))
    return values.astype(jnp.bfloat16).astype(jnp.float32)


def fill_table(shifts_ref, table_ref, rolled_ref):
    for q in range(16):
        first = pltpu.roll(shifts_ref[...], 16 * q, 1)
        second = pltpu.roll(shifts_ref[...], 16 * q + 8, 1)
        rolled_ref[16 * q : 16 * q + 16, :] = jnp.concatenate([first, second], 0).astype(jnp.bfloat16)
    for q in range(8):
        for n in range(8):
            for h in range(2):
                start = 128 * (n + 8 * h) - 256 * q + WIDTH
                table_ref[n, 256 * q : 256 * q + 256, 128 * h : 128 * h + 128] = rolled_ref[:, start : start + 128]


TILES = WIDTH // 128
GROUPS = 16


def position(owner, place):
    x, y, core = place >> 3, (place >> 1) & 3, place & 1
    along_x, along_y = (owner // SIDE - x) & 3, (owner % SIDE - y) & 3
    return jnp.where(core == 0, along_x * SIDE + along_y, along_y * SIDE + along_x)


def energy_kernel(place_ref, input_ref, given_ref, shifts_ref, *refs):
    held_ref, mask_ref, stats_ref, peak_ref, sems = refs
    last = (LAGS - 128 * (TILES - 1)) * GROUPS

    def fetch(j, size):
        return pltpu.make_async_copy(
            input_ref.at[pl.ds(j * 128 * GROUPS, size), :], held_ref.at[j, pl.ds(0, size), :], sems.at[j]
        )

    mask_copy = pltpu.make_async_copy(given_ref, mask_ref, sems.at[TILES])
    mask_copy.start()
    for j in range(TILES):
        fetch(j, 128 * GROUPS if j < TILES - 1 else last).start()
    held_ref[TILES - 1, last:, :] = jnp.zeros((128 * GROUPS - last, 128), jnp.bfloat16)

    def tile(j, carry):
        total, most = carry
        for b in range(8):
            values = held_ref[j, 256 * b : 256 * b + 256, :].astype(jnp.float32)
            squares = (values * values).reshape(16, GROUPS, 128)
            total += jnp.sum(squares, axis=0)
            most = jnp.maximum(most, jnp.max(squares, axis=0))
        return total, most

    def step(j, carry):
        fetch(j, 128 * GROUPS).wait()
        return tile(j, carry)

    zero = jnp.zeros((GROUPS, 128), jnp.float32)
    carry = lax.fori_loop(0, TILES - 1, step, (zero, zero))
    fetch(TILES - 1, last).wait()
    total, most = tile(TILES - 1, carry)
    mask_copy.wait()
    used = jnp.concatenate([mask_ref[:, 128 * t : 128 * t + 128] for t in range(4)], 0).astype(jnp.float32)
    total, most = total * used, most * used

    row = lax.broadcasted_iota(jnp.int32, (8, 128), 0)
    day = lax.broadcasted_iota(jnp.int32, (GROUPS, 128), 0) % DAYS
    stats = peaks = jnp.zeros((8, 128), jnp.float32)
    for d in range(DAYS):
        stats = jnp.where(row == d, jnp.sum(jnp.where(day == d, total, 0.0)), stats)
        stats = jnp.where(row == DAYS + d, jnp.sum(jnp.where(day == d, used, 0.0)), stats)
        peaks = jnp.where(row == d, jnp.max(jnp.where(day == d, most, 0.0)), peaks)
    peak_ref[...] = peaks
    stats_ref[...] = stats


def energies(place, correlations, mask, shifts):
    stored = correlations.reshape(DAYS, 4, 128, LAGS).transpose(3, 1, 0, 2).reshape(LAGS * GROUPS, 128)
    vmem, hbm = pl.BlockSpec(memory_space=pltpu.VMEM), pl.BlockSpec(memory_space=pltpu.HBM)
    return pl.pallas_call(
        energy_kernel,
        in_specs=[pl.BlockSpec(memory_space=pltpu.SMEM), hbm, hbm, vmem],
        out_specs=[vmem] * 4,
        out_shape=[
            jax.ShapeDtypeStruct((TILES, 128 * GROUPS, 128), jnp.bfloat16),
            jax.ShapeDtypeStruct(mask.shape, mask.dtype),
            jax.ShapeDtypeStruct((8, 128), jnp.float32),
            jax.ShapeDtypeStruct((8, 128), jnp.float32),
        ],
        scratch_shapes=[pltpu.SemaphoreType.DMA((TILES + 1,))],
        compiler_params=params(vmem_limit_bytes=12 * MB),
        name="energy",
    )(
        place,
        pltpu.with_memory_space_constraint(stored, pltpu.HBM),
        pltpu.with_memory_space_constraint(mask, pltpu.HBM),
        shifts,
    )


def rows_kernel(first_tile, last_tile, place_ref, held_ref, mask_ref, *refs):
    out_ref = refs[-1]
    place = place_ref[0]
    row = lax.broadcasted_iota(jnp.int32, (256, 256), 0)
    col = lax.broadcasted_iota(jnp.int32, (256, 256), 1)
    select = ((row // 16 == col % 16) & (row % 16 == col // 16)).astype(jnp.float32).astype(jnp.bfloat16)
    places = [position(owner, place) for owner in range(SIDE * SIDE)]

    def tile(j, carry):
        parts = []
        for b in range(4):
            first = held_ref[j, 512 * b : 512 * b + 256, :]
            second = held_ref[j, 512 * b + 256 : 512 * b + 512, :]
            parts.append(
                jnp.dot(select, jnp.concatenate([first, second], 1), preferred_element_type=jnp.float32)
            )
        for t in range(4):
            for d in range(DAYS):
                at = 16 * (t * DAYS + d)
                pieces = [p[at : at + 16, 128 * h : 128 * h + 128] for p in parts for h in range(2)]
                used = mask_ref[d : d + 1, 128 * t : 128 * t + 128].astype(jnp.float32)
                turned = (jnp.concatenate(pieces, 0) * used).astype(jnp.bfloat16).T
                for i in range(4):
                    lanes = pl.ds(pl.multiple_of(j * 128, 128), 128)
                    out_ref[places[t * 4 + i], d, :, lanes] = turned[OWNED * i : OWNED * i + OWNED, :]
        return carry

    lax.fori_loop(first_tile, last_tile, tile, 0)


def ordered_rows(place, held, mask, before=None):
    vmem = pl.BlockSpec(memory_space=pltpu.VMEM)
    tiles = (0, TILES // 2) if before is None else (TILES // 2, TILES)
    started = [] if before is None else [before]
    return pl.pallas_call(
        functools.partial(rows_kernel, *tiles),
        in_specs=[pl.BlockSpec(memory_space=pltpu.SMEM)] + [vmem] * (2 + len(started)),
        out_specs=vmem,
        out_shape=jax.ShapeDtypeStruct((SIDE * SIDE, DAYS, OWNED, WIDTH), jnp.bfloat16),
        input_output_aliases={3: 0} if started else {},
        compiler_params=params(vmem_limit_bytes=12 * MB),
        cost_estimate=pl.CostEstimate(flops=4 * 10**9, bytes_accessed=8 * MB, transcendentals=0),
        name="rows",
    )(place, held, mask, *started)


def kernel_table(shifts):
    vmem = pl.BlockSpec(memory_space=pltpu.VMEM)
    return pl.pallas_call(
        fill_table,
        in_specs=[vmem],
        out_specs=vmem,
        out_shape=jax.ShapeDtypeStruct((8, WIDTH, 256), jnp.bfloat16),
        scratch_shapes=[pltpu.VMEM((256, 2 * WIDTH), jnp.bfloat16)],
        compiler_params=params(vmem_limit_bytes=12 * MB),
        cost_estimate=pl.CostEstimate(flops=10**9, bytes_accessed=8 * MB, transcendentals=0),
        name="table",
    )(shifts)


def add_kernel(a_ref, b_ref, out_ref):
    out_ref[...] = a_ref[...] + b_ref[...]


def add(a, b):
    vmem = pl.BlockSpec(memory_space=pltpu.VMEM)
    return pl.pallas_call(
        add_kernel,
        in_specs=[vmem] * 2,
        out_specs=vmem,
        out_shape=jax.ShapeDtypeStruct(a.shape, a.dtype),
        compiler_params=params(vmem_limit_bytes=MB),
        name="add",
    )(a, b)


def terms_kernel(k, first, count, rows_ref, table_ref, stats_ref, others_ref, peak_ref, out_ref, even_ref, odd_ref):
    total = stats_ref[...] + others_ref[...]
    energy, used = total[:DAYS, :], total[DAYS:, :]
    weight = lax.rsqrt(energy / (LAGS * jnp.maximum(used, 1.0)) + 0.1)
    reach = weight * jnp.sqrt(peak_ref[:DAYS, :])
    bounds = [
        jnp.sum(reach, axis=0, keepdims=True),
        jnp.sum(jnp.minimum(1.0, 2.0 * reach), axis=0, keepdims=True),
        jnp.sum(jnp.minimum(1.0, 2.0 * KERNEL_SUM * reach), axis=0, keepdims=True),
    ]
    powers = [jnp.ceil(jnp.log(jnp.maximum(v, 1e-30) * 1.001) * 1.4426951) for v in bounds]
    scale = [TOP * jnp.exp2(-0.5 * p) for p in powers]
    row = lax.broadcasted_iota(jnp.int32, (8, 128), 0)
    exponents = jnp.where(row == 0, powers[0], jnp.where(row == 1, powers[1], powers[2])).astype(jnp.int32)
    for n in range(WORDS // 128):
        out_ref[count * QUANTITIES * OWNED :, 128 * n : 128 * n + 128] = exponents
    weights = [weight[d : d + 1, :] for d in range(DAYS)]
    floor = 0.25 / (weight * weight)
    floors = [floor[d : d + 1, :] for d in range(DAYS)]
    base = first * DAYS * OWNED

    def product(n, to_ref):
        to_ref[...] = jnp.dot(
            rows_ref[k, base : base + count * DAYS * OWNED, :], table_ref[n], preferred_element_type=jnp.float32
        )

    def finish_block(n, hilbert_ref):
        for l in range(count):
            codes = []
            for h in range(2):
                lanes = pl.ds(pl.multiple_of(n * 128 + h * WORDS, 128), 128)
                linear = real = imag = None
                for d in range(DAYS):
                    at = (l * DAYS + d) * OWNED
                    x = rows_ref[k, base + at : base + at + OWNED, lanes].astype(jnp.float32)
                    y = hilbert_ref[at : at + OWNED, 128 * h : 128 * h + 128]
                    inverse = lax.rsqrt(x * x + (y * y + floors[d]))
                    a, b = x * inverse, y * inverse
                    linear = x * weights[d] if d == 0 else linear + x * weights[d]
                    real = a if d == 0 else real + a
                    imag = b if d == 0 else imag + b
                codes.append([encode(v, scale[q]) for q, v in enumerate((linear, real, imag))])
            for q in range(QUANTITIES):
                at = (l * QUANTITIES + q) * OWNED
                out_ref[at : at + OWNED, pl.ds(pl.multiple_of(n * 128, 128), 128)] = pack(codes[0][q], codes[1][q])

    def step(i, carry):
        product(2 * i + 1, odd_ref)
        finish_block(2 * i, even_ref)
        product(2 * i + 2, even_ref)
        finish_block(2 * i + 1, odd_ref)
        return carry

    product(0, even_ref)
    lax.fori_loop(0, 3, step, 0)
    product(7, odd_ref)
    finish_block(6, even_ref)
    finish_block(7, odd_ref)


def terms(k, first, count, rows, table, *stats):
    vmem = pl.BlockSpec(memory_space=pltpu.VMEM)
    return pl.pallas_call(
        functools.partial(terms_kernel, k, first, count),
        in_specs=[vmem] * 5,
        out_specs=vmem,
        out_shape=jax.ShapeDtypeStruct((count * QUANTITIES * OWNED + 8, WORDS), jnp.int32),
        scratch_shapes=[pltpu.VMEM((count * DAYS * OWNED, 256), jnp.float32)] * 2,
        compiler_params=params(vmem_limit_bytes=24 * MB),
        cost_estimate=pl.CostEstimate(
            flops=2 * count * DAYS * OWNED * WIDTH * WIDTH, bytes_accessed=12 * MB, transcendentals=0
        ),
        name="terms",
    )(rows, table, *stats)


def decode(message_ref, at, exponent, cols):
    k = unit(exponent)
    low, high = unpack(message_ref[at : at + OWNED, cols])
    return low * k, high * k


def gather_kernel(cuts, blocks, *refs):
    refs, (out_ref, top_ref) = list(refs[:-2]), refs[-2:]
    messages = [[refs.pop(0) for _ in range(cut)] for cut in cuts]
    heads = [parts[0].shape[0] - 8 for parts in messages]
    top = None
    for parts, head in zip(messages, heads):
        exponents = parts[0][head : head + 8, :128]
        top = exponents if top is None else jnp.maximum(top, exponents)
    top_ref[...] = top
    for l in range(blocks):
        for j in range(WORDS // 128):
            cols = slice(128 * j, 128 * j + 128)
            for q in range(QUANTITIES):
                low = high = None
                for parts, head in zip(messages, heads):
                    each = blocks // len(parts)
                    at = (l % each * QUANTITIES + q) * OWNED
                    exponent = parts[0][head + q : head + q + 1, :128]
                    a, b = decode(parts[l // each], at, exponent, cols)
                    low = a if low is None else low + a
                    high = b if high is None else high + b
                at = (l * QUANTITIES + q) * OWNED
                out_ref[at : at + OWNED, cols] = low
                out_ref[at : at + OWNED, 128 * j + WORDS : 128 * j + WORDS + 128] = high


def gather(messages, blocks):
    vmem = pl.BlockSpec(memory_space=pltpu.VMEM)
    parts = [part for message in messages for part in message]
    return pl.pallas_call(
        functools.partial(gather_kernel, [len(message) for message in messages], blocks),
        in_specs=[vmem] * len(parts),
        out_specs=[vmem] * 2,
        out_shape=[
            jax.ShapeDtypeStruct((blocks * QUANTITIES * OWNED, WIDTH), jnp.float32),
            jax.ShapeDtypeStruct((8, 128), jnp.int32),
        ],
        compiler_params=params(vmem_limit_bytes=16 * MB),
        cost_estimate=pl.CostEstimate(flops=blocks * MB, bytes_accessed=2 * MB, transcendentals=0),
        name="gather",
    )(*parts)


def combine_kernel(l, sums_ref, top_ref, *refs):
    messages, out_ref = refs[:-1], refs[-1]
    heads = [message.shape[0] - 8 for message in messages]
    exponents = [message[head : head + 8, :128] for message, head in zip(messages, heads)]
    top = top_ref[...]
    for exponent in exponents:
        top = jnp.maximum(top, exponent)
    top = top + 2
    scale = jnp.exp2(-0.5 * top.astype(jnp.float32)) * TOP
    for j in range(WORDS // 128):
        cols = slice(128 * j, 128 * j + 128)
        for q in range(QUANTITIES):
            at = (l * QUANTITIES + q) * OWNED
            low = sums_ref[at : at + OWNED, cols]
            high = sums_ref[at : at + OWNED, 128 * j + WORDS : 128 * j + WORDS + 128]
            for message, head, exponent in zip(messages, heads, exponents):
                a, b = decode(message, at % head, exponent[q : q + 1, :], cols)
                low, high = low + a, high + b
            s = scale[q : q + 1, :]
            out_ref[q * OWNED : (q + 1) * OWNED, cols] = pack(encode(low, s), encode(high, s))
        out_ref[QUANTITIES * OWNED :, cols] = top


def combine(l, sums, top, messages):
    vmem = pl.BlockSpec(memory_space=pltpu.VMEM)
    return pl.pallas_call(
        functools.partial(combine_kernel, l),
        in_specs=[vmem] * (2 + len(messages)),
        out_specs=vmem,
        out_shape=jax.ShapeDtypeStruct((QUANTITIES * OWNED + 8, WORDS), jnp.int32),
        compiler_params=params(vmem_limit_bytes=16 * MB),
        cost_estimate=pl.CostEstimate(flops=2 * MB, bytes_accessed=2 * MB, transcendentals=0),
        name="combine",
    )(sums, top, *messages)


def finish_kernel(divisor_ref, sums_ref, message_ref, weighted_ref, linear_ref):
    inverse = 1.0 / divisor_ref[...]
    rows = QUANTITIES * OWNED
    exponents = message_ref[rows : rows + 8, :128]
    for j in range(WORDS // 128):
        cols = slice(128 * j, 128 * j + 128)
        pairs = [decode(message_ref, q * OWNED, exponents[q : q + 1, :], cols) for q in range(QUANTITIES)]
        for h in range(2):
            start = 128 * j + WORDS * h
            size = min(128, LAGS - start)
            linear, real, imag = [
                pairs[q][h] + sums_ref[q * OWNED : (q + 1) * OWNED, start : start + 128] for q in range(QUANTITIES)
            ]
            linear, real, imag = linear * inverse, real * inverse, imag * inverse
            weighted = linear * (real * real + imag * imag)
            linear_ref[:, start : start + size] = linear[:, :size]
            weighted_ref[:, start : start + size] = weighted[:, :size]


def finish(divisor, sums, message):
    vmem = pl.BlockSpec(memory_space=pltpu.VMEM)
    return pl.pallas_call(
        finish_kernel,
        in_specs=[vmem] * 3,
        out_specs=[vmem] * 2,
        out_shape=[jax.ShapeDtypeStruct((OWNED, LAGS), jnp.float32)] * 2,
        compiler_params=params(vmem_limit_bytes=16 * MB),
        name="finish",
    )(divisor, sums, message)


def shift(message, step, first):
    moves = []
    for x in range(SIDE):
        for y in range(SIDE):
            for pair in range(8):
                along_x = (pair % 2 == 0) == first
                to_x = (x + step) % SIDE if along_x else x
                to_y = y if along_x else (y + step) % SIDE
                moves.append(((x * SIDE + y) * 8 + pair, (to_x * SIDE + to_y) * 8 + pair))
    return lax.ppermute(message, ("day", "pair"), moves)


def trade(values, bit):
    moves = [(d * 8 + p, d * 8 + (p ^ bit)) for d in range(SIDE * SIDE) for p in range(8)]
    return lax.ppermute(values, ("day", "pair"), moves)


def stacks(correlations, mask, counts):
    place = (lax.axis_index("day") * 2 + lax.axis_index("pair") % 2).reshape(1)
    shifts = first_shifts()
    held, mask, stats, peak = energies(place, correlations, mask, shifts)
    others = trade(stats, 1)
    table = kernel_table(shifts)
    stats = add(stats, others)
    others = trade(stats, 2)
    rows = ordered_rows(place, held, mask)
    stats = add(stats, others)
    others = trade(stats, 6)
    rows = ordered_rows(place, held, mask, rows)
    rows = rows.reshape(SIDE, SIDE * DAYS * OWNED, WIDTH)

    def wide_step(k, first=0, count=SIDE):
        piece = terms(k, first, count, rows, table, stats, others, peak)
        return shift(piece, k, True) if k else piece

    def narrow_step(l):
        piece = combine(l, sums, top, [ahead, behind[l // 2]])
        return shift(piece, l, False) if l else piece

    far = [wide_step(2, 0, 2), wide_step(2, 2, 2)]
    ahead = wide_step(1)
    behind = [wide_step(3, 0, 2), wide_step(3, 2, 2)]
    own = wide_step(0)
    sums, top = gather([[own], far], SIDE)
    last, near, far, own = [narrow_step(l) for l in (2, 1, 3, 0)]
    sums, top = gather([[own], [near], [far]], 1)
    divisor = jnp.broadcast_to(jnp.maximum(counts.astype(jnp.float32), 1.0)[:, None], (OWNED, 128))
    return tuple(finish(divisor, sums, last))


def solution(mesh):
    placed = (P("day", "pair", None), P("day", "pair"), P(("pair", "day")))
    return jax.shard_map(
        stacks,
        mesh=mesh,
        in_specs=placed,
        out_specs=(P(("pair", "day"), None), P(("pair", "day"), None)),
        check_vma=False,
    )
```

```python
import functools

import jax
import jax.numpy as jnp
from jax import lax
from jax.experimental import pallas as pl
from jax.experimental.pallas import tpu as pltpu
from jax.sharding import PartitionSpec as P


LAGS = 2001
WIDTH = 2048
WORDS = WIDTH // 2
OWNED = 32
DAYS = 4
SIDE = 4
QUANTITIES = 3
TOP = 32766.0
KERNEL_SUM = 6.0
MB = 1 << 20


def params(**settings):
    return pltpu.CompilerParams(**{"vmem_limit_bytes": 32 * MB, **settings})


def encode(value, scale):
    root = value * lax.rsqrt(jnp.abs(value) + 1e-36)
    return (root * scale + 32768.5).astype(jnp.int32)


def pack(low, high):
    return low | (high << 16)


def unpack(word):
    low = (word & 0xFFFF).astype(jnp.float32) - 32768.0
    high = (lax.shift_right_logical(word, 16)).astype(jnp.float32) - 32768.0
    return low * jnp.abs(low), high * jnp.abs(high)


def tag(word, exponent):
    lane = lax.broadcasted_iota(jnp.int32, word.shape, 1)
    return jnp.where(lane == 127, pack(word & 0xFFFF, exponent.astype(jnp.int32) + 32768), word)


def tagged(message_ref, q):
    word = message_ref[q * OWNED : q * OWNED + 8, WORDS - 128 :]
    lane = lax.broadcasted_iota(jnp.int32, word.shape, 1)
    high = lax.shift_right_logical(word, 16).astype(jnp.float32) - 32768.0
    return jnp.max(jnp.where(lane == 127, high, -65536.0), axis=1, keepdims=True)[:1, :]


def unit(exponent):
    return jnp.exp2(exponent) * (1.0 / (TOP * TOP))


def first_shifts():
    row = lax.broadcasted_iota(jnp.int32, (8, 2 * WIDTH), 0)
    col = lax.broadcasted_iota(jnp.int32, (8, 2 * WIDTH), 1)
    offset = (col - row - WIDTH + 2 * LAGS) % LAGS
    offset = jnp.where(offset > LAGS // 2, offset - LAGS, offset)
    angle = jnp.pi * offset.astype(jnp.float32) / LAGS
    parity = 1.0 - 2.0 * (offset % 2).astype(jnp.float32)
    sine = jnp.where(offset == 0, 1.0, jnp.sin(angle))
    values = jnp.where(offset == 0, 0.0, (jnp.cos(angle) - parity) / (LAGS * sine))
    return values.astype(jnp.bfloat16).astype(jnp.float32)


def fill_table(shifts_ref, table_ref, rolled_ref):
    for q in range(16):
        first = pltpu.roll(shifts_ref[...], 16 * q, 1)
        second = pltpu.roll(shifts_ref[...], 16 * q + 8, 1)
        rolled_ref[16 * q : 16 * q + 16, :] = jnp.concatenate([first, second], 0).astype(jnp.bfloat16)
    for q in range(8):
        for n in range(8):
            for h in range(2):
                start = 128 * (n + 8 * h) - 256 * q + WIDTH
                table_ref[n, 256 * q : 256 * q + 256, 128 * h : 128 * h + 128] = rolled_ref[:, start : start + 128]


TILES = WIDTH // 128
GROUPS = 16


def position(owner, place):
    x, y, core = place >> 3, (place >> 1) & 3, place & 1
    along_x, along_y = (owner // SIDE - x) & 3, (owner % SIDE - y) & 3
    return jnp.where(core == 0, along_x * SIDE + along_y, along_y * SIDE + along_x)


def energy_kernel(place_ref, input_ref, given_ref, shifts_ref, *refs):
    held_ref, mask_ref, stats_ref, peak_ref, sems = refs
    last = (LAGS - 128 * (TILES - 1)) * GROUPS

    def fetch(j, size):
        return pltpu.make_async_copy(
            input_ref.at[pl.ds(j * 128 * GROUPS, size), :], held_ref.at[j, pl.ds(0, size), :], sems.at[j]
        )

    mask_copy = pltpu.make_async_copy(given_ref, mask_ref, sems.at[TILES])
    mask_copy.start()
    for j in range(TILES):
        fetch(j, 128 * GROUPS if j < TILES - 1 else last).start()
    held_ref[TILES - 1, last:, :] = jnp.zeros((128 * GROUPS - last, 128), jnp.bfloat16)

    def tile(j, carry):
        total, most = carry
        for b in range(8):
            values = held_ref[j, 256 * b : 256 * b + 256, :].astype(jnp.float32)
            squares = (values * values).reshape(16, GROUPS, 128)
            total += jnp.sum(squares, axis=0)
            most = jnp.maximum(most, jnp.max(squares, axis=0))
        return total, most

    def step(j, carry):
        fetch(j, 128 * GROUPS).wait()
        return tile(j, carry)

    zero = jnp.zeros((GROUPS, 128), jnp.float32)
    carry = lax.fori_loop(0, TILES - 1, step, (zero, zero))
    fetch(TILES - 1, last).wait()
    total, most = tile(TILES - 1, carry)
    mask_copy.wait()
    used = jnp.concatenate([mask_ref[:, 128 * t : 128 * t + 128] for t in range(4)], 0).astype(jnp.float32)
    total, most = total * used, most * used

    row = lax.broadcasted_iota(jnp.int32, (8, 128), 0)
    day = lax.broadcasted_iota(jnp.int32, (GROUPS, 128), 0) % DAYS
    stats = peaks = jnp.zeros((8, 128), jnp.float32)
    for d in range(DAYS):
        stats = jnp.where(row == d, jnp.sum(jnp.where(day == d, total, 0.0)), stats)
        stats = jnp.where(row == DAYS + d, jnp.sum(jnp.where(day == d, used, 0.0)), stats)
        peaks = jnp.where(row == d, jnp.max(jnp.where(day == d, most, 0.0)), peaks)
    peak_ref[...] = peaks
    stats_ref[...] = stats


def energies(place, correlations, mask, shifts):
    stored = correlations.reshape(DAYS, 4, 128, LAGS).transpose(3, 1, 0, 2).reshape(LAGS * GROUPS, 128)
    vmem, hbm = pl.BlockSpec(memory_space=pltpu.VMEM), pl.BlockSpec(memory_space=pltpu.HBM)
    return pl.pallas_call(
        energy_kernel,
        in_specs=[pl.BlockSpec(memory_space=pltpu.SMEM), hbm, hbm, vmem],
        out_specs=[vmem] * 4,
        out_shape=[
            jax.ShapeDtypeStruct((TILES, 128 * GROUPS, 128), jnp.bfloat16),
            jax.ShapeDtypeStruct(mask.shape, mask.dtype),
            jax.ShapeDtypeStruct((8, 128), jnp.float32),
            jax.ShapeDtypeStruct((8, 128), jnp.float32),
        ],
        scratch_shapes=[pltpu.SemaphoreType.DMA((TILES + 1,))],
        compiler_params=params(vmem_limit_bytes=12 * MB),
        name="energy",
    )(
        place,
        pltpu.with_memory_space_constraint(stored, pltpu.HBM),
        pltpu.with_memory_space_constraint(mask, pltpu.HBM),
        shifts,
    )


def rows_kernel(first_tile, last_tile, place_ref, held_ref, mask_ref, *refs):
    out_ref = refs[-1]
    place = place_ref[0]
    row = lax.broadcasted_iota(jnp.int32, (256, 256), 0)
    col = lax.broadcasted_iota(jnp.int32, (256, 256), 1)
    select = ((row // 16 == col % 16) & (row % 16 == col // 16)).astype(jnp.float32).astype(jnp.bfloat16)
    places = [position(owner, place) for owner in range(SIDE * SIDE)]

    def tile(j, carry):
        parts = []
        for b in range(4):
            first = held_ref[j, 512 * b : 512 * b + 256, :]
            second = held_ref[j, 512 * b + 256 : 512 * b + 512, :]
            parts.append(
                jnp.dot(select, jnp.concatenate([first, second], 1), preferred_element_type=jnp.float32)
            )
        for t in range(4):
            for d in range(DAYS):
                at = 16 * (t * DAYS + d)
                pieces = [p[at : at + 16, 128 * h : 128 * h + 128] for p in parts for h in range(2)]
                used = mask_ref[d : d + 1, 128 * t : 128 * t + 128].astype(jnp.float32)
                turned = (jnp.concatenate(pieces, 0) * used).astype(jnp.bfloat16).T
                for i in range(4):
                    lanes = pl.ds(pl.multiple_of(j * 128, 128), 128)
                    out_ref[places[t * 4 + i], d, :, lanes] = turned[OWNED * i : OWNED * i + OWNED, :]
        return carry

    lax.fori_loop(first_tile, last_tile, tile, 0)


def ordered_rows(place, held, mask, before=None):
    vmem = pl.BlockSpec(memory_space=pltpu.VMEM)
    tiles = (0, TILES // 2) if before is None else (TILES // 2, TILES)
    started = [] if before is None else [before]
    return pl.pallas_call(
        functools.partial(rows_kernel, *tiles),
        in_specs=[pl.BlockSpec(memory_space=pltpu.SMEM)] + [vmem] * (2 + len(started)),
        out_specs=vmem,
        out_shape=jax.ShapeDtypeStruct((SIDE * SIDE, DAYS, OWNED, WIDTH), jnp.bfloat16),
        input_output_aliases={3: 0} if started else {},
        compiler_params=params(vmem_limit_bytes=12 * MB),
        cost_estimate=pl.CostEstimate(flops=4 * 10**9, bytes_accessed=8 * MB, transcendentals=0),
        name="rows",
    )(place, held, mask, *started)


def kernel_table(shifts):
    vmem = pl.BlockSpec(memory_space=pltpu.VMEM)
    return pl.pallas_call(
        fill_table,
        in_specs=[vmem],
        out_specs=vmem,
        out_shape=jax.ShapeDtypeStruct((8, WIDTH, 256), jnp.bfloat16),
        scratch_shapes=[pltpu.VMEM((256, 2 * WIDTH), jnp.bfloat16)],
        compiler_params=params(vmem_limit_bytes=12 * MB),
        cost_estimate=pl.CostEstimate(flops=10**9, bytes_accessed=8 * MB, transcendentals=0),
        name="table",
    )(shifts)


def add_kernel(a_ref, b_ref, out_ref):
    out_ref[...] = a_ref[...] + b_ref[...]


def add(a, b):
    vmem = pl.BlockSpec(memory_space=pltpu.VMEM)
    return pl.pallas_call(
        add_kernel,
        in_specs=[vmem] * 2,
        out_specs=vmem,
        out_shape=jax.ShapeDtypeStruct(a.shape, a.dtype),
        compiler_params=params(vmem_limit_bytes=MB),
        name="add",
    )(a, b)


def terms_kernel(k, first, count, rows_ref, table_ref, stats_ref, others_ref, peak_ref, out_ref, even_ref, odd_ref):
    total = stats_ref[...] + others_ref[...]
    energy, used = total[:DAYS, :], total[DAYS:, :]
    weight = lax.rsqrt(energy / (LAGS * jnp.maximum(used, 1.0)) + 0.1)
    reach = weight * jnp.sqrt(peak_ref[:DAYS, :])
    bounds = [
        jnp.sum(reach, axis=0, keepdims=True),
        jnp.sum(jnp.minimum(1.0, 2.0 * reach), axis=0, keepdims=True),
        jnp.sum(jnp.minimum(1.0, 2.0 * KERNEL_SUM * reach), axis=0, keepdims=True),
    ]
    powers = [jnp.ceil(jnp.log(jnp.maximum(v, 1e-30) * 1.001) * 1.4426951) for v in bounds]
    scale = [TOP * jnp.exp2(-0.5 * p) for p in powers]
    weights = [weight[d : d + 1, :] for d in range(DAYS)]
    floor = 0.25 / (weight * weight)
    floors = [floor[d : d + 1, :] for d in range(DAYS)]
    base = first * DAYS * OWNED

    def product(n, to_ref):
        to_ref[...] = jnp.dot(
            rows_ref[k, base : base + count * DAYS * OWNED, :], table_ref[n], preferred_element_type=jnp.float32
        )

    def finish_block(n, hilbert_ref, tags=False):
        for l in range(count):
            codes = []
            for h in range(2):
                lanes = pl.ds(pl.multiple_of(n * 128 + h * WORDS, 128), 128)
                linear = real = imag = None
                for d in range(DAYS):
                    at = (l * DAYS + d) * OWNED
                    x = rows_ref[k, base + at : base + at + OWNED, lanes].astype(jnp.float32)
                    y = hilbert_ref[at : at + OWNED, 128 * h : 128 * h + 128]
                    inverse = lax.rsqrt(x * x + (y * y + floors[d]))
                    a, b = x * inverse, y * inverse
                    linear = x * weights[d] if d == 0 else linear + x * weights[d]
                    real = a if d == 0 else real + a
                    imag = b if d == 0 else imag + b
                codes.append([encode(v, scale[q]) for q, v in enumerate((linear, real, imag))])
            for q in range(QUANTITIES):
                at = (l * QUANTITIES + q) * OWNED
                word = pack(codes[0][q], codes[1][q])
                if tags:
                    word = tag(word, powers[q])
                out_ref[at : at + OWNED, pl.ds(pl.multiple_of(n * 128, 128), 128)] = word

    def step(i, carry):
        product(2 * i + 1, odd_ref)
        finish_block(2 * i, even_ref)
        product(2 * i + 2, even_ref)
        finish_block(2 * i + 1, odd_ref)
        return carry

    product(0, even_ref)
    lax.fori_loop(0, 3, step, 0)
    product(7, odd_ref)
    finish_block(6, even_ref)
    finish_block(7, odd_ref, True)


def terms(k, first, count, rows, table, *stats):
    vmem = pl.BlockSpec(memory_space=pltpu.VMEM)
    return pl.pallas_call(
        functools.partial(terms_kernel, k, first, count),
        in_specs=[vmem] * 5,
        out_specs=vmem,
        out_shape=jax.ShapeDtypeStruct((count * QUANTITIES * OWNED, WORDS), jnp.int32),
        scratch_shapes=[pltpu.VMEM((count * DAYS * OWNED, 256), jnp.float32)] * 2,
        compiler_params=params(vmem_limit_bytes=24 * MB),
        cost_estimate=pl.CostEstimate(
            flops=2 * count * DAYS * OWNED * WIDTH * WIDTH, bytes_accessed=12 * MB, transcendentals=0
        ),
        name="terms",
    )(rows, table, *stats)


def decode(message_ref, at, exponent, cols):
    k = unit(exponent)
    low, high = unpack(message_ref[at : at + OWNED, cols])
    return low * k, high * k


def gather_kernel(cuts, blocks, *refs):
    refs, (out_ref, top_ref) = list(refs[:-2]), refs[-2:]
    messages = [[refs.pop(0) for _ in range(cut)] for cut in cuts]
    exponents = [[tagged(parts[0], q) for q in range(QUANTITIES)] for parts in messages]
    row = lax.broadcasted_iota(jnp.int32, (8, 128), 0)
    top = [functools.reduce(jnp.maximum, [e[q] for e in exponents]) for q in range(QUANTITIES)]
    top_ref[...] = jnp.where(row == 0, top[0], jnp.where(row == 1, top[1], top[2]))
    for l in range(blocks):
        for j in range(WORDS // 128):
            cols = slice(128 * j, 128 * j + 128)
            for q in range(QUANTITIES):
                low = high = None
                for parts, exponent in zip(messages, exponents):
                    each = blocks // len(parts)
                    at = (l % each * QUANTITIES + q) * OWNED
                    a, b = decode(parts[l // each], at, exponent[q], cols)
                    low = a if low is None else low + a
                    high = b if high is None else high + b
                at = (l * QUANTITIES + q) * OWNED
                out_ref[at : at + OWNED, cols] = low
                out_ref[at : at + OWNED, 128 * j + WORDS : 128 * j + WORDS + 128] = high


def gather(messages, blocks):
    vmem = pl.BlockSpec(memory_space=pltpu.VMEM)
    parts = [part for message in messages for part in message]
    return pl.pallas_call(
        functools.partial(gather_kernel, [len(message) for message in messages], blocks),
        in_specs=[vmem] * len(parts),
        out_specs=[vmem] * 2,
        out_shape=[
            jax.ShapeDtypeStruct((blocks * QUANTITIES * OWNED, WIDTH), jnp.float32),
            jax.ShapeDtypeStruct((8, 128), jnp.float32),
        ],
        compiler_params=params(vmem_limit_bytes=16 * MB),
        cost_estimate=pl.CostEstimate(flops=blocks * MB, bytes_accessed=2 * MB, transcendentals=0),
        name="gather",
    )(*parts)


def combine_kernel(l, sums_ref, top_ref, *refs):
    messages, out_ref = refs[:-1], refs[-1]
    exponents = [[tagged(message, q) for q in range(QUANTITIES)] for message in messages]
    tops = []
    for q in range(QUANTITIES):
        tops.append(functools.reduce(jnp.maximum, [e[q] for e in exponents], top_ref[q : q + 1, :]) + 2.0)
    scale = [jnp.exp2(-0.5 * top) * TOP for top in tops]
    for j in range(WORDS // 128):
        cols = slice(128 * j, 128 * j + 128)
        for q in range(QUANTITIES):
            at = (l * QUANTITIES + q) * OWNED
            low = sums_ref[at : at + OWNED, cols]
            high = sums_ref[at : at + OWNED, 128 * j + WORDS : 128 * j + WORDS + 128]
            for message, exponent in zip(messages, exponents):
                a, b = decode(message, at % message.shape[0], exponent[q], cols)
                low, high = low + a, high + b
            word = pack(encode(low, scale[q]), encode(high, scale[q]))
            if j == WORDS // 128 - 1:
                word = tag(word, tops[q])
            out_ref[q * OWNED : (q + 1) * OWNED, cols] = word


def combine(l, sums, top, messages):
    vmem = pl.BlockSpec(memory_space=pltpu.VMEM)
    return pl.pallas_call(
        functools.partial(combine_kernel, l),
        in_specs=[vmem] * (2 + len(messages)),
        out_specs=vmem,
        out_shape=jax.ShapeDtypeStruct((QUANTITIES * OWNED, WORDS), jnp.int32),
        compiler_params=params(vmem_limit_bytes=16 * MB),
        cost_estimate=pl.CostEstimate(flops=2 * MB, bytes_accessed=2 * MB, transcendentals=0),
        name="combine",
    )(sums, top, *messages)


def finish_kernel(divisor_ref, sums_ref, message_ref, weighted_ref, linear_ref):
    inverse = 1.0 / divisor_ref[...]
    exponents = [tagged(message_ref, q) for q in range(QUANTITIES)]
    for j in range(WORDS // 128):
        cols = slice(128 * j, 128 * j + 128)
        pairs = [decode(message_ref, q * OWNED, exponents[q], cols) for q in range(QUANTITIES)]
        for h in range(2):
            start = 128 * j + WORDS * h
            size = min(128, LAGS - start)
            linear, real, imag = [
                pairs[q][h] + sums_ref[q * OWNED : (q + 1) * OWNED, start : start + 128] for q in range(QUANTITIES)
            ]
            linear, real, imag = linear * inverse, real * inverse, imag * inverse
            weighted = linear * (real * real + imag * imag)
            linear_ref[:, start : start + size] = linear[:, :size]
            weighted_ref[:, start : start + size] = weighted[:, :size]


def finish(divisor, sums, message):
    vmem = pl.BlockSpec(memory_space=pltpu.VMEM)
    return pl.pallas_call(
        finish_kernel,
        in_specs=[vmem] * 3,
        out_specs=[vmem] * 2,
        out_shape=[jax.ShapeDtypeStruct((OWNED, LAGS), jnp.float32)] * 2,
        compiler_params=params(vmem_limit_bytes=16 * MB),
        name="finish",
    )(divisor, sums, message)


def shift(message, step, first):
    moves = []
    for x in range(SIDE):
        for y in range(SIDE):
            for pair in range(8):
                along_x = (pair % 2 == 0) == first
                to_x = (x + step) % SIDE if along_x else x
                to_y = y if along_x else (y + step) % SIDE
                moves.append(((x * SIDE + y) * 8 + pair, (to_x * SIDE + to_y) * 8 + pair))
    return lax.ppermute(message, ("day", "pair"), moves)


def trade(values, bit):
    moves = [(d * 8 + p, d * 8 + (p ^ bit)) for d in range(SIDE * SIDE) for p in range(8)]
    return lax.ppermute(values, ("day", "pair"), moves)


def stacks(correlations, mask, counts):
    place = (lax.axis_index("day") * 2 + lax.axis_index("pair") % 2).reshape(1)
    shifts = first_shifts()
    held, mask, stats, peak = energies(place, correlations, mask, shifts)
    others = trade(stats, 1)
    table = kernel_table(shifts)
    stats = add(stats, others)
    others = trade(stats, 2)
    rows = ordered_rows(place, held, mask)
    stats = add(stats, others)
    others = trade(stats, 6)
    rows = ordered_rows(place, held, mask, rows)
    rows = rows.reshape(SIDE, SIDE * DAYS * OWNED, WIDTH)

    def wide_step(k, first=0, count=SIDE):
        piece = terms(k, first, count, rows, table, stats, others, peak)
        return shift(piece, k, True) if k else piece

    def narrow_step(l):
        piece = combine(l, sums, top, [ahead, behind[l // 2]])
        return shift(piece, l, False) if l else piece

    far = [wide_step(2, 0, 2), wide_step(2, 2, 2)]
    ahead = wide_step(1)
    behind = [wide_step(3, 0, 2), wide_step(3, 2, 2)]
    own = wide_step(0)
    sums, top = gather([[own], far], SIDE)
    last, near, far, own = [narrow_step(l) for l in (2, 1, 3, 0)]
    sums, top = gather([[own], [near], [far]], 1)
    divisor = jnp.broadcast_to(jnp.maximum(counts.astype(jnp.float32), 1.0)[:, None], (OWNED, 128))
    return tuple(finish(divisor, sums, last))


def solution(mesh):
    placed = (P("day", "pair", None), P("day", "pair"), P(("pair", "day")))
    return jax.shard_map(
        stacks,
        mesh=mesh,
        in_specs=placed,
        out_specs=(P(("pair", "day"), None), P(("pair", "day"), None)),
        check_vma=False,
    )
```

```python
import functools

import jax
import jax.numpy as jnp
from jax import lax
from jax.experimental import pallas as pl
from jax.experimental.pallas import tpu as pltpu
from jax.sharding import PartitionSpec as P


LAGS = 2001
WIDTH = 2048
WORDS = WIDTH // 2
OWNED = 32
DAYS = 4
SIDE = 4
QUANTITIES = 3
TOP = 32766.0
KERNEL_SUM = 6.0
MB = 1 << 20


def params(**settings):
    return pltpu.CompilerParams(**{"vmem_limit_bytes": 32 * MB, **settings})


def encode(value, scale):
    root = value * lax.rsqrt(jnp.abs(value) + 1e-36)
    return (root * scale + 32768.5).astype(jnp.int32)


def pack(low, high):
    return low | (high << 16)


def unpack(word):
    low = (word & 0xFFFF).astype(jnp.float32) - 32768.0
    high = (lax.shift_right_logical(word, 16)).astype(jnp.float32) - 32768.0
    return low * jnp.abs(low), high * jnp.abs(high)


def tag(word, exponent):
    lane = lax.broadcasted_iota(jnp.int32, word.shape, 1)
    return jnp.where(lane == 127, pack(word & 0xFFFF, exponent.astype(jnp.int32) + 32768), word)


def tagged(message_ref, q):
    word = message_ref[q * OWNED : q * OWNED + 8, WORDS - 128 :]
    lane = lax.broadcasted_iota(jnp.int32, word.shape, 1)
    high = lax.shift_right_logical(word, 16).astype(jnp.float32) - 32768.0
    return jnp.max(jnp.where(lane == 127, high, -65536.0), axis=1, keepdims=True)[:1, :]


def unit(exponent):
    return jnp.exp2(exponent) * (1.0 / (TOP * TOP))


def first_shifts():
    row = lax.broadcasted_iota(jnp.int32, (8, 2 * WIDTH), 0)
    col = lax.broadcasted_iota(jnp.int32, (8, 2 * WIDTH), 1)
    offset = (col - row - WIDTH + 2 * LAGS) % LAGS
    offset = jnp.where(offset > LAGS // 2, offset - LAGS, offset)
    angle = jnp.pi * offset.astype(jnp.float32) / LAGS
    parity = 1.0 - 2.0 * (offset % 2).astype(jnp.float32)
    sine = jnp.where(offset == 0, 1.0, jnp.sin(angle))
    values = jnp.where(offset == 0, 0.0, (jnp.cos(angle) - parity) / (LAGS * sine))
    return values.astype(jnp.bfloat16).astype(jnp.float32)


def fill_table(shifts_ref, table_ref, rolled_ref):
    for q in range(16):
        first = pltpu.roll(shifts_ref[...], 16 * q, 1)
        second = pltpu.roll(shifts_ref[...], 16 * q + 8, 1)
        rolled_ref[16 * q : 16 * q + 16, :] = jnp.concatenate([first, second], 0).astype(jnp.bfloat16)
    for q in range(8):
        for n in range(8):
            for h in range(2):
                start = 128 * (n + 8 * h) - 256 * q + WIDTH
                table_ref[n, 256 * q : 256 * q + 256, 128 * h : 128 * h + 128] = rolled_ref[:, start : start + 128]


TILES = WIDTH // 128
GROUPS = 16


def position(owner, place):
    x, y, core = place >> 3, (place >> 1) & 3, place & 1
    along_x, along_y = (owner // SIDE - x) & 3, (owner % SIDE - y) & 3
    return jnp.where(core == 0, along_x * SIDE + along_y, along_y * SIDE + along_x)


def energy_kernel(place_ref, input_ref, given_ref, shifts_ref, *refs):
    held_ref, mask_ref, stats_ref, peak_ref, sems = refs
    last = (LAGS - 128 * (TILES - 1)) * GROUPS

    def fetch(j, size):
        return pltpu.make_async_copy(
            input_ref.at[pl.ds(j * 128 * GROUPS, size), :], held_ref.at[j, pl.ds(0, size), :], sems.at[j]
        )

    mask_copy = pltpu.make_async_copy(given_ref, mask_ref, sems.at[TILES])
    mask_copy.start()
    for j in range(TILES):
        fetch(j, 128 * GROUPS if j < TILES - 1 else last).start()
    held_ref[TILES - 1, last:, :] = jnp.zeros((128 * GROUPS - last, 128), jnp.bfloat16)

    def tile(j, carry):
        total, most = carry
        for b in range(8):
            values = held_ref[j, 256 * b : 256 * b + 256, :].astype(jnp.float32)
            squares = (values * values).reshape(16, GROUPS, 128)
            total += jnp.sum(squares, axis=0)
            most = jnp.maximum(most, jnp.max(squares, axis=0))
        return total, most

    def step(j, carry):
        fetch(j, 128 * GROUPS).wait()
        return tile(j, carry)

    zero = jnp.zeros((GROUPS, 128), jnp.float32)
    carry = lax.fori_loop(0, TILES - 1, step, (zero, zero))
    fetch(TILES - 1, last).wait()
    total, most = tile(TILES - 1, carry)
    mask_copy.wait()
    used = jnp.concatenate([mask_ref[:, 128 * t : 128 * t + 128] for t in range(4)], 0).astype(jnp.float32)
    total, most = total * used, most * used

    row = lax.broadcasted_iota(jnp.int32, (8, 128), 0)
    day = lax.broadcasted_iota(jnp.int32, (GROUPS, 128), 0) % DAYS
    stats = peaks = jnp.zeros((8, 128), jnp.float32)
    for d in range(DAYS):
        stats = jnp.where(row == d, jnp.sum(jnp.where(day == d, total, 0.0)), stats)
        stats = jnp.where(row == DAYS + d, jnp.sum(jnp.where(day == d, used, 0.0)), stats)
        peaks = jnp.where(row == d, jnp.max(jnp.where(day == d, most, 0.0)), peaks)
    peak_ref[...] = peaks
    stats_ref[...] = stats


def energies(place, correlations, mask, shifts):
    stored = correlations.reshape(DAYS, 4, 128, LAGS).transpose(3, 1, 0, 2).reshape(LAGS * GROUPS, 128)
    vmem, hbm = pl.BlockSpec(memory_space=pltpu.VMEM), pl.BlockSpec(memory_space=pltpu.HBM)
    return pl.pallas_call(
        energy_kernel,
        in_specs=[pl.BlockSpec(memory_space=pltpu.SMEM), hbm, hbm, vmem],
        out_specs=[vmem] * 4,
        out_shape=[
            jax.ShapeDtypeStruct((TILES, 128 * GROUPS, 128), jnp.bfloat16),
            jax.ShapeDtypeStruct(mask.shape, mask.dtype),
            jax.ShapeDtypeStruct((8, 128), jnp.float32),
            jax.ShapeDtypeStruct((8, 128), jnp.float32),
        ],
        scratch_shapes=[pltpu.SemaphoreType.DMA((TILES + 1,))],
        compiler_params=params(vmem_limit_bytes=12 * MB),
        name="energy",
    )(
        place,
        pltpu.with_memory_space_constraint(stored, pltpu.HBM),
        pltpu.with_memory_space_constraint(mask, pltpu.HBM),
        shifts,
    )


def rows_kernel(first_tile, last_tile, place_ref, held_ref, mask_ref, *refs):
    out_ref = refs[-1]
    place = place_ref[0]
    row = lax.broadcasted_iota(jnp.int32, (256, 256), 0)
    col = lax.broadcasted_iota(jnp.int32, (256, 256), 1)
    select = ((row // 16 == col % 16) & (row % 16 == col // 16)).astype(jnp.float32).astype(jnp.bfloat16)
    places = [position(owner, place) for owner in range(SIDE * SIDE)]

    def tile(j, carry):
        parts = []
        for b in range(4):
            first = held_ref[j, 512 * b : 512 * b + 256, :]
            second = held_ref[j, 512 * b + 256 : 512 * b + 512, :]
            parts.append(
                jnp.dot(select, jnp.concatenate([first, second], 1), preferred_element_type=jnp.float32)
            )
        for t in range(4):
            for d in range(DAYS):
                at = 16 * (t * DAYS + d)
                pieces = [p[at : at + 16, 128 * h : 128 * h + 128] for p in parts for h in range(2)]
                used = mask_ref[d : d + 1, 128 * t : 128 * t + 128].astype(jnp.float32)
                turned = (jnp.concatenate(pieces, 0) * used).astype(jnp.bfloat16).T
                for i in range(4):
                    lanes = pl.ds(pl.multiple_of(j * 128, 128), 128)
                    out_ref[places[t * 4 + i], d, :, lanes] = turned[OWNED * i : OWNED * i + OWNED, :]
        return carry

    lax.fori_loop(first_tile, last_tile, tile, 0)


def ordered_rows(place, held, mask, before=None):
    vmem = pl.BlockSpec(memory_space=pltpu.VMEM)
    tiles = (0, TILES // 2) if before is None else (TILES // 2, TILES)
    started = [] if before is None else [before]
    return pl.pallas_call(
        functools.partial(rows_kernel, *tiles),
        in_specs=[pl.BlockSpec(memory_space=pltpu.SMEM)] + [vmem] * (2 + len(started)),
        out_specs=vmem,
        out_shape=jax.ShapeDtypeStruct((SIDE * SIDE, DAYS, OWNED, WIDTH), jnp.bfloat16),
        input_output_aliases={3: 0} if started else {},
        compiler_params=params(vmem_limit_bytes=12 * MB),
        cost_estimate=pl.CostEstimate(flops=4 * 10**9, bytes_accessed=8 * MB, transcendentals=0),
        name="rows",
    )(place, held, mask, *started)


def kernel_table(shifts):
    vmem = pl.BlockSpec(memory_space=pltpu.VMEM)
    return pl.pallas_call(
        fill_table,
        in_specs=[vmem],
        out_specs=vmem,
        out_shape=jax.ShapeDtypeStruct((8, WIDTH, 256), jnp.bfloat16),
        scratch_shapes=[pltpu.VMEM((256, 2 * WIDTH), jnp.bfloat16)],
        compiler_params=params(vmem_limit_bytes=12 * MB),
        cost_estimate=pl.CostEstimate(flops=10**9, bytes_accessed=8 * MB, transcendentals=0),
        name="table",
    )(shifts)


def add_kernel(a_ref, b_ref, out_ref):
    out_ref[...] = a_ref[...] + b_ref[...]


def add(a, b):
    vmem = pl.BlockSpec(memory_space=pltpu.VMEM)
    return pl.pallas_call(
        add_kernel,
        in_specs=[vmem] * 2,
        out_specs=vmem,
        out_shape=jax.ShapeDtypeStruct(a.shape, a.dtype),
        compiler_params=params(vmem_limit_bytes=MB),
        name="add",
    )(a, b)


def terms_kernel(k, first, count, rows_ref, table_ref, stats_ref, others_ref, peak_ref, out_ref, even_ref, odd_ref):
    total = stats_ref[...] + others_ref[...]
    energy, used = total[:DAYS, :], total[DAYS:, :]
    weight = lax.rsqrt(energy / (LAGS * jnp.maximum(used, 1.0)) + 0.1)
    reach = weight * jnp.sqrt(peak_ref[:DAYS, :])
    bounds = [
        jnp.sum(reach, axis=0, keepdims=True),
        jnp.sum(jnp.minimum(1.0, 2.0 * reach), axis=0, keepdims=True),
        jnp.sum(jnp.minimum(1.0, 2.0 * KERNEL_SUM * reach), axis=0, keepdims=True),
    ]
    powers = [jnp.ceil(jnp.log(jnp.maximum(v, 1e-30) * 1.001) * 1.4426951) for v in bounds]
    scale = [TOP * jnp.exp2(-0.5 * p) for p in powers]
    weights = [weight[d : d + 1, :] for d in range(DAYS)]
    floor = 0.25 / (weight * weight)
    floors = [floor[d : d + 1, :] for d in range(DAYS)]
    base = first * DAYS * OWNED

    def product(n, to_ref):
        to_ref[...] = jnp.dot(
            rows_ref[k, base : base + count * DAYS * OWNED, :], table_ref[n], preferred_element_type=jnp.float32
        )

    def finish_block(n, hilbert_ref, tags=False):
        for l in range(count):
            codes = []
            for h in range(2):
                lanes = pl.ds(pl.multiple_of(n * 128 + h * WORDS, 128), 128)
                linear = real = imag = None
                for d in range(DAYS):
                    at = (l * DAYS + d) * OWNED
                    x = rows_ref[k, base + at : base + at + OWNED, lanes].astype(jnp.float32)
                    y = hilbert_ref[at : at + OWNED, 128 * h : 128 * h + 128]
                    inverse = lax.rsqrt(x * x + (y * y + floors[d]))
                    a, b = x * inverse, y * inverse
                    linear = x * weights[d] if d == 0 else linear + x * weights[d]
                    real = a if d == 0 else real + a
                    imag = b if d == 0 else imag + b
                codes.append([encode(v, scale[q]) for q, v in enumerate((linear, real, imag))])
            for q in range(QUANTITIES):
                at = (l * QUANTITIES + q) * OWNED
                word = pack(codes[0][q], codes[1][q])
                if tags:
                    word = tag(word, powers[q])
                out_ref[at : at + OWNED, pl.ds(pl.multiple_of(n * 128, 128), 128)] = word

    def step(i, carry):
        product(2 * i + 1, odd_ref)
        finish_block(2 * i, even_ref)
        product(2 * i + 2, even_ref)
        finish_block(2 * i + 1, odd_ref)
        return carry

    product(0, even_ref)
    lax.fori_loop(0, 3, step, 0)
    product(7, odd_ref)
    finish_block(6, even_ref)
    finish_block(7, odd_ref, True)


def terms(k, first, count, rows, table, *stats):
    vmem = pl.BlockSpec(memory_space=pltpu.VMEM)
    return pl.pallas_call(
        functools.partial(terms_kernel, k, first, count),
        in_specs=[vmem] * 5,
        out_specs=vmem,
        out_shape=jax.ShapeDtypeStruct((count * QUANTITIES * OWNED, WORDS), jnp.int32),
        scratch_shapes=[pltpu.VMEM((count * DAYS * OWNED, 256), jnp.float32)] * 2,
        compiler_params=params(vmem_limit_bytes=24 * MB),
        cost_estimate=pl.CostEstimate(
            flops=2 * count * DAYS * OWNED * WIDTH * WIDTH, bytes_accessed=12 * MB, transcendentals=0
        ),
        name="terms",
    )(rows, table, *stats)


def decode(message_ref, at, exponent, cols):
    k = unit(exponent)
    low, high = unpack(message_ref[at : at + OWNED, cols])
    return low * k, high * k


def gather_kernel(cuts, blocks, *refs):
    refs, (out_ref, top_ref) = list(refs[:-2]), refs[-2:]
    messages = [[refs.pop(0) for _ in range(cut)] for cut in cuts]
    exponents = [[tagged(parts[0], q) for q in range(QUANTITIES)] for parts in messages]
    row = lax.broadcasted_iota(jnp.int32, (8, 128), 0)
    top = [functools.reduce(jnp.maximum, [e[q] for e in exponents]) for q in range(QUANTITIES)]
    top_ref[...] = jnp.where(row == 0, top[0], jnp.where(row == 1, top[1], top[2]))
    for l in range(blocks):
        for j in range(WORDS // 128):
            cols = slice(128 * j, 128 * j + 128)
            for q in range(QUANTITIES):
                low = high = None
                for parts, exponent in zip(messages, exponents):
                    each = blocks // len(parts)
                    at = (l % each * QUANTITIES + q) * OWNED
                    a, b = decode(parts[l // each], at, exponent[q], cols)
                    low = a if low is None else low + a
                    high = b if high is None else high + b
                at = (l * QUANTITIES + q) * OWNED
                out_ref[at : at + OWNED, cols] = low
                out_ref[at : at + OWNED, 128 * j + WORDS : 128 * j + WORDS + 128] = high


def gather(messages, blocks):
    vmem = pl.BlockSpec(memory_space=pltpu.VMEM)
    parts = [part for message in messages for part in message]
    return pl.pallas_call(
        functools.partial(gather_kernel, [len(message) for message in messages], blocks),
        in_specs=[vmem] * len(parts),
        out_specs=[vmem] * 2,
        out_shape=[
            jax.ShapeDtypeStruct((blocks * QUANTITIES * OWNED, WIDTH), jnp.float32),
            jax.ShapeDtypeStruct((8, 128), jnp.float32),
        ],
        compiler_params=params(vmem_limit_bytes=16 * MB),
        cost_estimate=pl.CostEstimate(flops=blocks * MB, bytes_accessed=2 * MB, transcendentals=0),
        name="gather",
    )(*parts)


def combine_kernel(l, sums_ref, top_ref, *refs):
    messages, out_ref = refs[:-1], refs[-1]
    exponents = [[tagged(message, q) for q in range(QUANTITIES)] for message in messages]
    tops = []
    for q in range(QUANTITIES):
        tops.append(functools.reduce(jnp.maximum, [e[q] for e in exponents], top_ref[q : q + 1, :]) + 2.0)
    scale = [jnp.exp2(-0.5 * top) * TOP for top in tops]
    for j in range(WORDS // 128):
        cols = slice(128 * j, 128 * j + 128)
        for q in range(QUANTITIES):
            at = (l * QUANTITIES + q) * OWNED
            low = sums_ref[at : at + OWNED, cols]
            high = sums_ref[at : at + OWNED, 128 * j + WORDS : 128 * j + WORDS + 128]
            for message, exponent in zip(messages, exponents):
                a, b = decode(message, at % message.shape[0], exponent[q], cols)
                low, high = low + a, high + b
            word = pack(encode(low, scale[q]), encode(high, scale[q]))
            if j == WORDS // 128 - 1:
                word = tag(word, tops[q])
            out_ref[q * OWNED : (q + 1) * OWNED, cols] = word


def combine(l, sums, top, messages):
    vmem = pl.BlockSpec(memory_space=pltpu.VMEM)
    return pl.pallas_call(
        functools.partial(combine_kernel, l),
        in_specs=[vmem] * (2 + len(messages)),
        out_specs=vmem,
        out_shape=jax.ShapeDtypeStruct((QUANTITIES * OWNED, WORDS), jnp.int32),
        compiler_params=params(vmem_limit_bytes=16 * MB),
        cost_estimate=pl.CostEstimate(flops=2 * MB, bytes_accessed=2 * MB, transcendentals=0),
        name="combine",
    )(sums, top, *messages)


def finish_kernel(divisor_ref, sums_ref, *refs):
    messages, (weighted_ref, linear_ref) = refs[:-2], refs[-2:]
    inverse = 1.0 / divisor_ref[...]
    exponents = [[tagged(message, q) for q in range(QUANTITIES)] for message in messages]
    for j in range(WORDS // 128):
        cols = slice(128 * j, 128 * j + 128)
        pairs = []
        for q in range(QUANTITIES):
            both = [decode(message, q * OWNED, e[q], cols) for message, e in zip(messages, exponents)]
            pairs.append([sum(each[1:], each[0]) for each in zip(*both)])
        for h in range(2):
            start = 128 * j + WORDS * h
            size = min(128, LAGS - start)
            linear, real, imag = [
                pairs[q][h] + sums_ref[q * OWNED : (q + 1) * OWNED, start : start + 128] for q in range(QUANTITIES)
            ]
            linear, real, imag = linear * inverse, real * inverse, imag * inverse
            weighted = linear * (real * real + imag * imag)
            linear_ref[:, start : start + size] = linear[:, :size]
            weighted_ref[:, start : start + size] = weighted[:, :size]


def finish(divisor, sums, messages):
    vmem = pl.BlockSpec(memory_space=pltpu.VMEM)
    return pl.pallas_call(
        finish_kernel,
        in_specs=[vmem] * (2 + len(messages)),
        out_specs=[vmem] * 2,
        out_shape=[jax.ShapeDtypeStruct((OWNED, LAGS), jnp.float32)] * 2,
        compiler_params=params(vmem_limit_bytes=16 * MB),
        name="finish",
    )(divisor, sums, *messages)


def shift(message, step, first):
    moves = []
    for x in range(SIDE):
        for y in range(SIDE):
            for pair in range(8):
                along_x = (pair % 2 == 0) == first
                to_x = (x + step) % SIDE if along_x else x
                to_y = y if along_x else (y + step) % SIDE
                moves.append(((x * SIDE + y) * 8 + pair, (to_x * SIDE + to_y) * 8 + pair))
    return lax.ppermute(message, ("day", "pair"), moves)


def trade(values, bit):
    moves = [(d * 8 + p, d * 8 + (p ^ bit)) for d in range(SIDE * SIDE) for p in range(8)]
    return lax.ppermute(values, ("day", "pair"), moves)


def stacks(correlations, mask, counts):
    place = (lax.axis_index("day") * 2 + lax.axis_index("pair") % 2).reshape(1)
    shifts = first_shifts()
    held, mask, stats, peak = energies(place, correlations, mask, shifts)
    others = trade(stats, 1)
    table = kernel_table(shifts)
    stats = add(stats, others)
    others = trade(stats, 2)
    rows = ordered_rows(place, held, mask)
    stats = add(stats, others)
    others = trade(stats, 6)
    rows = ordered_rows(place, held, mask, rows)
    rows = rows.reshape(SIDE, SIDE * DAYS * OWNED, WIDTH)

    def wide_step(k, first=0, count=SIDE):
        piece = terms(k, first, count, rows, table, stats, others, peak)
        return shift(piece, k, True) if k else piece

    def narrow_step(l):
        piece = combine(l, sums, top, [ahead, behind[l // 2]])
        return shift(piece, l, False) if l else piece

    far = [wide_step(2, 0, 2), wide_step(2, 2, 2)]
    ahead = wide_step(1)
    behind = [wide_step(3, 0, 2), wide_step(3, 2, 2)]
    own = wide_step(0)
    sums, top = gather([[own], far], SIDE)
    last, near, far, own = [narrow_step(l) for l in (2, 1, 3, 0)]
    sums, top = gather([[own], [last]], 1)
    divisor = jnp.broadcast_to(jnp.maximum(counts.astype(jnp.float32), 1.0)[:, None], (OWNED, 128))
    return tuple(finish(divisor, sums, [near, far]))


def solution(mesh):
    placed = (P("day", "pair", None), P("day", "pair"), P(("pair", "day")))
    return jax.shard_map(
        stacks,
        mesh=mesh,
        in_specs=placed,
        out_specs=(P(("pair", "day"), None), P(("pair", "day"), None)),
        check_vma=False,
    )
```
